32 devices in a mesh: node: 16 (over z, y, core), harm: 2 (over x).
Axes of the slice: x: 2, y: 2, z: 4, core: 2. Of those that a mesh axis runs over, the one named last changes fastest.
Arguments:
- spectrum: float32 [128, 3, 98304], P('harm', None, 'node'), may hold values from -2 to 2
- source: float32 [128, 3, 98304], P('harm', None, 'node'), may hold values from -4 to 4
- coupling: bfloat16 [768, 4, 128, 128], P('node'), may hold values from -0.75 to 0.75
- capacitance: float32 [98304], P('node'), may hold values from 0.5 to 4
- saturation: float32 [98304], P('node'), may hold values from 0.1 to 1
- steepness: float32 [98304], P('node'), may hold values from 0.5 to 4
- junction: float32 [98304], P('node'), may hold values from 0.2 to 2
- halo_list: int32 [16, 4, 4], replicated, may hold values from 0 to 47, as said below
- neighbour_slot: int32 [768, 4], P('node'), may hold values from 0 to 64, as said below
Outputs:
- residual: float32 [128, 3, 98304], P('harm', None, 'node')
The draws below stay inside these ranges and needn't reach their ends.
Inputs may be any that keep to these rules, and one draw needn't show every extreme that they name: `halo_list`: row [m, j] lists 4 distinct blocks of device m, by index among its 48 blocks, needed by the device at index m + o_j along node, o = (-2, -1, 1, 2). `neighbour_slot`: column 0 of block b is b's own index among the 48 blocks of its device d. Other entries v: own block v if v < 48; block halo_list[m, j, s] of device m = d - o_j if v = 48 + j * 4 + s, only where m lies on the mesh; v = 64 is an empty entry. Every such slot of a device whose sender lies on the mesh is named by some entry of the device.
All inputs are finite; a program needn't handle non-finite values.
Results may differ from the reference program's by a relative error of at most 0.0025.
Values may be sent and summed in bfloat16 or wider, within the bound.
A program may use at most 128 MiB of HBM per device.

```python
import math
import jax
import jax.numpy as jnp
from jax import lax

HARMS = 64
SPEC = 128
BLK = 128
NNZ = 4
SLOTS = 4
POINTS = 3
NB_DEV = 48
NBLK = 768
NODES = 98304
N_NODE = 16


def draw_halo_list(key, part):
    keys = jax.random.split(key, N_NODE * 4)
    chosen = jax.vmap(lambda single: jax.random.permutation(single, NB_DEV)[:SLOTS])(keys)
    return chosen.reshape(N_NODE, 4, SLOTS).astype(jnp.int32)


def draw_neighbour_slot(key, part):
    empty_slot = NB_DEV + 4 * SLOTS
    entries = NB_DEV * (NNZ - 1)

    def per_device(device_key, device):
        first_key, second_key = jax.random.split(device_key)
        halo_slots = NB_DEV + jnp.arange(4 * SLOTS, dtype=jnp.int32)
        others = jax.random.randint(first_key, (entries - 4 * SLOTS,), 0, empty_slot + 1, dtype=jnp.int32)
        mixed = jax.random.permutation(second_key, jnp.concatenate([halo_slots, others]))
        direction = jnp.clip((mixed - NB_DEV) // SLOTS, 0, 3)
        offset = direction - 2 + (direction >= 2).astype(jnp.int32)
        sender = device - offset
        remote = (mixed >= NB_DEV) & (mixed < empty_slot)
        broken = remote & ((sender < 0) | (sender >= N_NODE))
        mixed = jnp.where(broken, empty_slot, mixed)
        own_column = jnp.arange(NB_DEV, dtype=jnp.int32)[:, None]
        return jnp.concatenate([own_column, mixed.reshape(NB_DEV, NNZ - 1)], axis=1)
    device_keys = jax.random.split(key, N_NODE)
    table = jax.vmap(per_device)(device_keys, jnp.arange(N_NODE, dtype=jnp.int32))
    return table.reshape(N_NODE * NB_DEV, NNZ).astype(jnp.int32)


def shard_levels(own_key, dims, cuts, least, top_value):
    factor_of = 1.0
    for dim, blocks in cuts:
        steps = jax.random.uniform(jax.random.fold_in(jax.random.fold_in(own_key, 6), dim), (blocks,), jnp.float32, least / len(cuts), top_value / len(cuts))
        factor_of = factor_of * jnp.repeat(jnp.exp(steps), dims[dim] // blocks).reshape((-1,) + (1,) * (len(dims) - 1 - dim))
    return factor_of


def centred(key, extent, spread, reach, cuts=(), kind=jnp.bfloat16):
    values = jax.random.normal(key, extent, jnp.float32) * spread
    if len(cuts) > 0:
        values = shard_levels(key, extent, cuts, -0.22, 0.18) * values
    return jnp.clip(values, min=-reach, max=reach).astype(kind)


def setup_inputs(seed: int = 0) -> dict:
    key_list = jax.random.split(jax.random.key(seed), 10)
    return {
        "spectrum": centred(key_list[0], (SPEC, POINTS, NODES), 0.15, 2.0, ((0, 2), (2, 16)), jnp.float32),
        "source": centred(key_list[1], (SPEC, POINTS, NODES), 0.3, 4.0, ((0, 2), (2, 16)), jnp.float32),
        "coupling": centred(key_list[2], (NBLK, NNZ, BLK, BLK), (NNZ * BLK // 8) ** -0.5, 0.75, ((0, 16),)),
        "capacitance": jnp.clip(jnp.exp(math.log(4.0) - 2.0794415 * jax.random.uniform(key_list[3], (NODES,), jnp.float32) ** shard_levels(key_list[3], (NODES,), ((0, 16),), -0.2, 0.2)), 0.5, 4.0),
        "saturation": jnp.clip(jnp.exp(math.log(1.0) - 2.3025851 * jax.random.uniform(key_list[4], (NODES,), jnp.float32) ** shard_levels(key_list[4], (NODES,), ((0, 16),), -0.2, 0.2)), 0.1, 1.0),
        "steepness": jnp.clip(jnp.exp(math.log(4.0) - 2.0794415 * jax.random.uniform(key_list[5], (NODES,), jnp.float32) ** shard_levels(key_list[5], (NODES,), ((0, 16),), -0.2, 0.2)), 0.5, 4.0),
        "junction": jnp.clip(jnp.exp(math.log(2.0) - 2.3025851 * jax.random.uniform(key_list[6], (NODES,), jnp.float32) ** shard_levels(key_list[6], (NODES,), ((0, 16),), -0.2, 0.2)), 0.2, 2.0),
        "halo_list": draw_halo_list(jax.random.fold_in(key_list[9], 71), 0),
        "neighbour_slot": draw_neighbour_slot(jax.random.fold_in(key_list[9], 71), 0),
    }


LOG_TWO = 0.6931471805599453

def synthesize(spectra):
    halfway = SPEC // 2
    cosines = spectra[0::2]
    sines = spectra[1::2]
    real_part = jnp.concatenate([cosines[:1] * SPEC, cosines[1:] * halfway, sines[:1] * SPEC], axis=0)
    zero_row = jnp.zeros_like(sines[:1])
    imag_part = jnp.concatenate([zero_row, -sines[1:] * halfway, zero_row], axis=0)
    return jnp.fft.irfft(real_part + 1j * imag_part, n=SPEC, axis=0).astype(jnp.float32)

def analyze(samples):
    halfway = SPEC // 2
    spectra = jnp.fft.rfft(samples, axis=0)
    lowest = spectra[0].real / SPEC
    highest = spectra[halfway].real / SPEC
    cosines = jnp.concatenate([lowest[None], 2.0 * spectra[1:halfway].real / SPEC], axis=0)
    sines = jnp.concatenate([highest[None], -2.0 * spectra[1:halfway].imag / SPEC], axis=0)
    return jnp.stack([cosines, sines], axis=1).reshape(SPEC, samples.shape[1]).astype(jnp.float32)

def derivative(spectra):
    pulsation = jnp.arange(SPEC // 2, dtype=jnp.float32)[:, None] / HARMS
    cosines = spectra[0::2]
    sines = spectra[1::2]
    return jnp.stack([pulsation * sines, -pulsation * cosines], axis=1).reshape(spectra.shape)

def single_level(spectrum, source, coupling, capacitance, saturation, steepness, junction, halo_list, neighbour_slot):
    rounded = spectrum.astype(jnp.bfloat16)
    blocks = rounded.reshape(SPEC, NBLK, BLK).transpose(1, 0, 2)
    offsets = jnp.array([-2, -1, 1, 2], dtype=jnp.int32)
    empty_slot = NB_DEV + 4 * SLOTS

    def per_device(device):
        slots = lax.dynamic_slice_in_dim(neighbour_slot, device * NB_DEV, NB_DEV, 0)
        relative = jnp.clip(slots - NB_DEV, 0, 4 * SLOTS - 1)
        direction = relative // SLOTS
        position = relative % SLOTS
        sender = jnp.clip(device - offsets[direction], 0, N_NODE - 1)
        remote = sender * NB_DEV + halo_list[sender, direction, position]
        global_id = jnp.where(slots < NB_DEV, device * NB_DEV + slots, remote)
        global_id = jnp.where(slots == empty_slot, 0, global_id).astype(jnp.int32)
        keep = (slots != empty_slot).astype(jnp.float32)
        picked = blocks[global_id].astype(jnp.float32) * keep[:, :, None, None]
        matrices = lax.dynamic_slice_in_dim(coupling, device * NB_DEV, NB_DEV, 0).astype(jnp.float32)
        return jnp.einsum('bksj,bkij->bsi', picked, matrices, precision=lax.Precision.HIGHEST)
    coupled = lax.map(per_device, jnp.arange(N_NODE, dtype=jnp.int32))
    coupled = coupled.reshape(NBLK, SPEC, BLK).transpose(1, 0, 2).reshape(SPEC, NODES)
    voltage = synthesize(spectrum)
    current = saturation * (jax.nn.softplus(steepness * voltage) - LOG_TWO)
    charge = junction * voltage / jnp.sqrt(1.0 + voltage * voltage)
    current_spec = analyze(current)
    charge_spec = analyze(charge)
    return coupled + derivative(capacitance * spectrum) + current_spec + derivative(charge_spec) - source

def reference(spectrum, source, coupling, capacitance, saturation, steepness, junction, halo_list, neighbour_slot):
    levels = []
    for level in range(POINTS):
        levels.append(single_level(spectrum[:, level], source[:, level], coupling, capacitance, saturation, steepness, junction, halo_list, neighbour_slot))
    return jnp.stack(levels, axis=1)
```

```python
import functools

import jax
import jax.numpy as jnp
import numpy as np
from jax import lax
from jax.experimental import pallas as pl
from jax.experimental.pallas import tpu as pltpu
from jax.sharding import PartitionSpec as P

LOG_TWO = 0.6931471805599453
OFFSETS = (-2, -1, 1, 2)
LANES = 128
VMEM_BYTES = 36 << 20
MESH = pl.DeviceIdType.MESH


def fourier_tables(length, shares):
    rows = length // shares
    sample = np.arange(length)[:, None]
    column = np.arange(length)[None, :]
    angle = 2.0 * np.pi / length * (column // 2 * sample % length)
    table = np.where(column % 2 == 1, np.sin(angle), np.cos(angle))
    table = np.where(column == 1, np.where(sample % 2 == 0, 1.0, -1.0), table)
    weights = np.where(np.arange(length) < 2, 1.0, 2.0) / length
    analysis = table.T * weights[:, None]
    pulsation = np.arange(length // 2)[:, None, None] / (length // 2)
    pairs = analysis.reshape(length // 2, 2, length)
    slope = np.concatenate([pulsation * pairs[:, 1:], -pulsation * pairs[:, :1]], axis=1)
    both = np.concatenate([analysis, slope.reshape(length, length)], axis=1)
    table = table.astype(np.float32)
    high = table.astype(jnp.bfloat16)
    low = (table - high.astype(np.float32)).astype(jnp.bfloat16)
    order = [
        np.concatenate([np.arange(rows) + (me - by) % shares * rows for by in range(shares)])
        for me in range(shares)
    ]
    synthesis = np.stack([np.concatenate([high[:, o], low[:, o]], axis=1) for o in order])
    return synthesis, both.astype(jnp.bfloat16).reshape(shares, rows, 2 * length)


def kernel(
    unit,
    list_ref,
    slot_ref,
    x_hbm,
    source_hbm,
    coupling_hbm,
    synthesis_hbm,
    analysis_hbm,
    capacitance_hbm,
    saturation_hbm,
    steepness_hbm,
    junction_hbm,
    out_ref,
    x_ref,
    coupling_ref,
    synthesis_ref,
    analysis_ref,
    scale_ref,
    pool_ref,
    arrived_ref,
    packed_ref,
    halo_ref,
    x_sem,
    local_sem,
    send_sem,
    recv_sem,
    halo_send_sem,
    halo_recv_sem,
):
    points, rows, nodes = x_ref.shape
    blocks = nodes // LANES
    width = unit * LANES
    chunks = blocks // unit
    count, slots = coupling_ref.shape[1], list_ref.shape[1]
    shares, devices = lax.axis_size("harm"), lax.axis_size("node")
    me, place = lax.axis_index("harm"), lax.axis_index("node")
    length = rows * shares

    def on_mesh(device):
        return jnp.logical_and(device >= 0, device < devices)

    def columns(chunk):
        return pl.ds(pl.multiple_of(chunk * width, width), width)

    def load(chunk):
        span = columns(chunk)
        return pltpu.make_async_copy(
            x_hbm.at[:, :, span], x_ref.at[:, :, span], x_sem.at[chunk]
        )

    def exchange(chunk, by):
        part = pl.ds(chunk * unit, unit)
        return pltpu.make_async_remote_copy(
            src_ref=pool_ref.at[part],
            dst_ref=arrived_ref.at[by - 1, part],
            send_sem=send_sem.at[by - 1, chunk],
            recv_sem=recv_sem.at[by - 1, chunk],
            device_id={"harm": lax.rem(me + by, shares)},
            device_id_type=MESH,
        )

    def halo(direction, device):
        return pltpu.make_async_remote_copy(
            src_ref=packed_ref.at[direction],
            dst_ref=halo_ref.at[direction],
            send_sem=halo_send_sem.at[direction],
            recv_sem=halo_recv_sem.at[direction],
            device_id={"node": device},
            device_id_type=MESH,
        )

    barrier = pltpu.get_barrier_semaphore()
    for by in range(1, shares):
        pl.semaphore_signal(
            barrier, inc=1, device_id={"harm": lax.rem(me + by, shares)}, device_id_type=MESH
        )
    greeted = shares - 1
    for offset in OFFSETS:
        there = on_mesh(place + offset)
        greeted = greeted + there.astype(jnp.int32)

        @pl.when(there)
        def _():
            pl.semaphore_signal(
                barrier, inc=1, device_id={"node": place + offset}, device_id_type=MESH
            )

    def start_load(chunk, carry):
        load(chunk).start()
        return carry

    lax.fori_loop(0, chunks, start_load, 0)
    local = [
        pltpu.make_async_copy(source, target, local_sem.at[i])
        for i, (source, target) in enumerate(
            [
                (source_hbm, out_ref),
                (coupling_hbm, coupling_ref),
                (capacitance_hbm, scale_ref.at[0]),
                (saturation_hbm, scale_ref.at[1]),
                (steepness_hbm, scale_ref.at[2]),
                (junction_hbm, scale_ref.at[3]),
                (synthesis_hbm.at[me], synthesis_ref),
                (analysis_hbm.at[me], analysis_ref),
            ]
        )
    ]
    for copy in local:
        copy.start()

    def round_chunk(chunk):
        load(chunk).wait()
        for inner in range(unit):
            block = chunk * unit + inner
            span = pl.ds(pl.multiple_of(block * LANES, LANES), LANES)
            for point in range(points):
                pool_ref[block, point * rows : (point + 1) * rows, :] = x_ref[
                    point, :, span
                ].astype(jnp.bfloat16)

    def send(chunk):
        for by in range(1, shares):
            exchange(chunk, by).start()

    round_chunk(0)
    pl.semaphore_wait(barrier, greeted)

    def advance(chunk, carry):
        round_chunk(chunk)
        send(chunk - 1)
        return carry

    lax.fori_loop(1, chunks, advance, 0)
    for direction in range(len(OFFSETS)):
        for slot in range(slots):
            packed_ref[direction, slot] = pool_ref[list_ref[direction, slot, place]]
    send(chunks - 1)
    for direction, offset in enumerate(OFFSETS):

        @pl.when(on_mesh(place + offset))
        def _():
            halo(direction, place + offset).start()

    pool_ref[blocks + len(OFFSETS) * slots] = jnp.zeros(pool_ref.shape[1:], pool_ref.dtype)
    for copy in local:
        copy.wait()
    for direction, offset in enumerate(OFFSETS):
        first = blocks + direction * slots
        there = on_mesh(place - offset)

        @pl.when(there)
        def _():
            halo(direction, place - offset).wait_recv()
            for slot in range(slots):
                pool_ref[first + slot] = halo_ref[direction, slot]

        @pl.when(jnp.logical_not(there))
        def _():
            for slot in range(slots):
                pool_ref[first + slot] = jnp.zeros(pool_ref.shape[1:], pool_ref.dtype)

    row = me * rows + lax.broadcasted_iota(jnp.int32, (rows, LANES), 0)
    even = row % 2 == 0
    rate = (row // 2).astype(jnp.float32) * (2.0 / length)
    rate = jnp.where(even, rate, -rate)

    def couple(block, carry):
        gathered = jnp.concatenate([pool_ref[slot_ref[k, block]] for k in range(count)], axis=1)
        matrix = jnp.concatenate([coupling_ref[block, k] for k in range(count)], axis=1)
        coupled = lax.dot_general(
            gathered, matrix, (((1,), (1,)), ((), ())), preferred_element_type=jnp.float32
        )
        scaled = rate * scale_ref[0, pl.ds(block, 1), :]
        span = pl.ds(pl.multiple_of(block * LANES, LANES), LANES)
        for point in range(points):
            values = x_ref[point, :, span]
            other = jnp.where(even, pltpu.roll(values, rows - 1, 0), pltpu.roll(values, 1, 0))
            out_ref[point, :, span] = (
                coupled[point * rows : (point + 1) * rows]
                + scaled * other
                - out_ref[point, :, span]
            )
        return carry

    lax.fori_loop(0, blocks, couple, 0, unroll=unit)

    def nonlinear(chunk, carry):
        for by in range(1, shares):
            exchange(chunk, by).wait_recv()
        ids = [chunk * unit + inner for inner in range(unit)]

        def scale(index):
            parts = [scale_ref[index, pl.ds(block, 1), :] for block in ids]
            return jnp.concatenate(parts, axis=1)

        saturation, steepness, junction = scale(1), scale(2), scale(3)
        span = columns(chunk)
        for point in range(points):
            held = slice(point * rows, (point + 1) * rows)
            spectra = [jnp.concatenate([pool_ref[block, held, :] for block in ids], axis=1)]
            for by in range(1, shares):
                spectra.append(
                    jnp.concatenate([arrived_ref[by - 1, block, held, :] for block in ids], axis=1)
                )
            stacked = jnp.concatenate(spectra + spectra, axis=0)
            voltage = jnp.dot(synthesis_ref[...], stacked, preferred_element_type=jnp.float32)
            drive = steepness * voltage
            softplus = jnp.maximum(drive, 0.0) + jnp.log(1.0 + jnp.exp(-jnp.abs(drive)))
            current = (saturation * (softplus - LOG_TWO)).astype(jnp.bfloat16)
            charge = (junction * voltage * lax.rsqrt(1.0 + voltage * voltage)).astype(jnp.bfloat16)
            samples = jnp.concatenate([current, charge], axis=0)
            out_ref[point, :, span] += jnp.dot(
                analysis_ref[...], samples, preferred_element_type=jnp.float32
            )
        return carry

    lax.fori_loop(0, chunks, nonlinear, 0)

    def drain(chunk, carry):
        for by in range(1, shares):
            exchange(chunk, by).wait_send()
        return carry

    lax.fori_loop(0, chunks, drain, 0)
    for direction, offset in enumerate(OFFSETS):

        @pl.when(on_mesh(place + offset))
        def _():
            halo(direction, place + offset).wait_send()


def local_part(
    spectrum,
    source,
    coupling,
    capacitance,
    saturation,
    steepness,
    junction,
    halo_list,
    neighbour_slot,
):
    rows, points, nodes = spectrum.shape
    shares = lax.axis_size("harm")
    length = rows * shares
    blocks = nodes // LANES
    unit = 2 if blocks % 2 == 0 else 1
    chunks = blocks // unit
    slots, count = halo_list.shape[2], neighbour_slot.shape[1]
    directions = len(OFFSETS)
    height = points * rows
    x = jnp.transpose(spectrum, (1, 0, 2))
    injected = jnp.transpose(source, (1, 0, 2))
    synthesis, analysis = (jnp.asarray(t) for t in fourier_tables(length, shares))
    scales = [v.reshape(blocks, LANES) for v in (capacitance, saturation, steepness, junction)]
    smem = pl.BlockSpec(memory_space=pltpu.SMEM)
    hbm = pl.BlockSpec(memory_space=pltpu.HBM)
    bf16, f32 = jnp.bfloat16, jnp.float32
    total = pl.pallas_call(
        functools.partial(kernel, unit),
        in_specs=[smem, smem] + [hbm] * 9,
        out_specs=pl.BlockSpec(memory_space=pltpu.VMEM),
        out_shape=pltpu.VMEM((points, rows, nodes), f32),
        scratch_shapes=[
            pltpu.VMEM((points, rows, nodes), f32),
            pltpu.VMEM((blocks, count, LANES, LANES), bf16),
            pltpu.VMEM((length, 2 * length), bf16),
            pltpu.VMEM((rows, 2 * length), bf16),
            pltpu.VMEM((4, blocks, LANES), f32),
            pltpu.VMEM((blocks + directions * slots + 1, height, LANES), bf16),
            pltpu.VMEM((shares - 1, blocks, height, LANES), bf16),
            pltpu.VMEM((directions, slots, height, LANES), bf16),
            pltpu.VMEM((directions, slots, height, LANES), bf16),
            pltpu.SemaphoreType.DMA((chunks,)),
            pltpu.SemaphoreType.DMA((8,)),
            pltpu.SemaphoreType.DMA((shares - 1, chunks)),
            pltpu.SemaphoreType.DMA((shares - 1, chunks)),
            pltpu.SemaphoreType.DMA((directions,)),
            pltpu.SemaphoreType.DMA((directions,)),
        ],
        compiler_params=pltpu.CompilerParams(
            collective_id=0, has_side_effects=True, vmem_limit_bytes=VMEM_BYTES
        ),
        cost_estimate=pl.CostEstimate(
            flops=2 * height * nodes * (count * LANES + 3 * length),
            bytes_accessed=coupling.size * 2 + 3 * x.size * 4,
            transcendentals=0,
        ),
        name="residual",
    )(
        jnp.transpose(halo_list, (1, 2, 0)),
        neighbour_slot.T,
        x,
        injected,
        coupling,
        synthesis,
        analysis,
        *scales,
    )
    return jnp.transpose(total, (1, 0, 2))


def solution(mesh):
    in_specs = (
        P("harm", None, "node"),
        P("harm", None, "node"),
        P("node", None, None, None),
        P("node"),
        P("node"),
        P("node"),
        P("node"),
        P(),
        P("node", None),
    )
    return jax.shard_map(
        local_part, mesh=mesh, in_specs=in_specs, out_specs=P("harm", None, "node"), check_vma=False
    )
```

```python
import functools

import jax
import jax.numpy as jnp
import numpy as np
from jax import lax
from jax.experimental import pallas as pl
from jax.experimental.pallas import tpu as pltpu
from jax.sharding import PartitionSpec as P

LOG_TWO = 0.6931471805599453
OFFSETS = (-2, -1, 1, 2)
LANES = 128
VMEM_BYTES = 36 << 20
MESH = pl.DeviceIdType.MESH


def fourier_tables(length, shares):
    rows = length // shares
    sample = np.arange(length)[:, None]
    column = np.arange(length)[None, :]
    angle = 2.0 * np.pi / length * (column // 2 * sample % length)
    table = np.where(column % 2 == 1, np.sin(angle), np.cos(angle))
    table = np.where(column == 1, np.where(sample % 2 == 0, 1.0, -1.0), table)
    weights = np.where(np.arange(length) < 2, 1.0, 2.0) / length
    analysis = table.T * weights[:, None]
    pulsation = np.arange(length // 2)[:, None, None] / (length // 2)
    pairs = analysis.reshape(length // 2, 2, length)
    slope = np.concatenate([pulsation * pairs[:, 1:], -pulsation * pairs[:, :1]], axis=1)
    both = np.concatenate([analysis, slope.reshape(length, length)], axis=1)
    table = table.astype(np.float32)
    high = table.astype(jnp.bfloat16)
    low = (table - high.astype(np.float32)).astype(jnp.bfloat16)
    order = [
        np.concatenate([np.arange(rows) + (me - by) % shares * rows for by in range(shares)])
        for me in range(shares)
    ]
    synthesis = np.stack([np.concatenate([high[:, o], low[:, o]], axis=1) for o in order])
    return synthesis, both.astype(jnp.bfloat16).reshape(shares, rows, 2 * length)


def evaluate(spectra, synthesis, analysis, saturation, steepness, junction):
    stacked = jnp.concatenate(spectra + spectra, axis=0)
    voltage = jnp.dot(synthesis, stacked, preferred_element_type=jnp.float32)
    drive = steepness * voltage
    softplus = jnp.maximum(drive, 0.0) + jnp.log(1.0 + jnp.exp(-jnp.abs(drive)))
    current = (saturation * (softplus - LOG_TWO)).astype(jnp.bfloat16)
    charge = (junction * voltage * lax.rsqrt(1.0 + voltage * voltage)).astype(jnp.bfloat16)
    samples = jnp.concatenate([current, charge], axis=0)
    return jnp.dot(analysis, samples, preferred_element_type=jnp.float32)


def widen(scale_ref, index, blocks):
    parts = [scale_ref[index, pl.ds(block, 1), :] for block in blocks]
    return jnp.concatenate(parts, axis=1)


def finish_kernel(pieces, total_ref, tail_ref, synthesis_ref, analysis_ref, scale_ref, out_hbm, last_ref, sem):
    points, rows, nodes = total_ref.shape
    shares, unit = tail_ref.shape[:2]
    blocks = nodes // LANES
    done = nodes - unit * LANES
    copies = []
    for point in range(points):
        for piece in range(pieces):
            part = (point, slice(piece * rows // pieces, (piece + 1) * rows // pieces), slice(0, done))
            copies.append(
                pltpu.make_async_copy(
                    total_ref.at[part], out_hbm.at[part], sem.at[point * pieces + piece]
                )
            )
    for copy in copies:
        copy.start()
    ids = range(blocks - unit, blocks)
    scales = [widen(scale_ref, index, ids) for index in (1, 2, 3)]
    for point in range(points):
        held = slice(point * rows, (point + 1) * rows)
        spectra = [
            jnp.concatenate([tail_ref[share, inner, held, :] for inner in range(unit)], axis=1)
            for share in range(shares)
        ]
        last_ref[point] = total_ref[point, :, done:] + evaluate(
            spectra, synthesis_ref[...], analysis_ref[...], *scales
        )
    copy = pltpu.make_async_copy(last_ref, out_hbm.at[:, :, done:], sem.at[points * pieces])
    copy.start()
    for each in copies + [copy]:
        each.wait()


def kernel(
    unit,
    list_hbm,
    slot_hbm,
    x_hbm,
    source_hbm,
    coupling_hbm,
    synthesis_hbm,
    analysis_hbm,
    capacitance_hbm,
    saturation_hbm,
    steepness_hbm,
    junction_hbm,
    out_ref,
    tail_ref,
    synthesis_ref,
    analysis_ref,
    scale_ref,
    list_ref,
    slot_ref,
    x_ref,
    coupling_ref,
    pool_ref,
    arrived_ref,
    packed_ref,
    halo_ref,
    x_sem,
    local_sem,
    send_sem,
    recv_sem,
    halo_send_sem,
    halo_recv_sem,
):
    points, rows, nodes = x_ref.shape
    blocks = nodes // LANES
    width = unit * LANES
    chunks = blocks // unit
    count, slots = coupling_ref.shape[1], list_ref.shape[1]
    shares, devices = lax.axis_size("harm"), lax.axis_size("node")
    me, place = lax.axis_index("harm"), lax.axis_index("node")
    length = rows * shares

    def on_mesh(device):
        return jnp.logical_and(device >= 0, device < devices)

    def columns(chunk):
        return pl.ds(pl.multiple_of(chunk * width, width), width)

    def load(chunk):
        span = columns(chunk)
        return pltpu.make_async_copy(
            x_hbm.at[:, :, span], x_ref.at[:, :, span], x_sem.at[chunk]
        )

    def exchange(chunk, by):
        part = pl.ds(chunk * unit, unit)
        return pltpu.make_async_remote_copy(
            src_ref=pool_ref.at[part],
            dst_ref=arrived_ref.at[by - 1, part],
            send_sem=send_sem.at[by - 1, chunk],
            recv_sem=recv_sem.at[by - 1, chunk],
            device_id={"harm": lax.rem(me + by, shares)},
            device_id_type=MESH,
        )

    def halo(direction, device):
        return pltpu.make_async_remote_copy(
            src_ref=packed_ref.at[direction],
            dst_ref=halo_ref.at[direction],
            send_sem=halo_send_sem.at[direction],
            recv_sem=halo_recv_sem.at[direction],
            device_id={"node": device},
            device_id_type=MESH,
        )

    barrier = pltpu.get_barrier_semaphore()
    for by in range(1, shares):
        pl.semaphore_signal(
            barrier, inc=1, device_id={"harm": lax.rem(me + by, shares)}, device_id_type=MESH
        )
    greeted = shares - 1
    for offset in OFFSETS:
        there = on_mesh(place + offset)
        greeted = greeted + there.astype(jnp.int32)

        @pl.when(there)
        def _():
            pl.semaphore_signal(
                barrier, inc=1, device_id={"node": place + offset}, device_id_type=MESH
            )

    def start_load(chunk, carry):
        load(chunk).start()
        return carry

    lax.fori_loop(0, chunks, start_load, 0)
    local = [
        pltpu.make_async_copy(source, target, local_sem.at[i])
        for i, (source, target) in enumerate(
            [
                (list_hbm, list_ref),
                (slot_hbm, slot_ref),
                (source_hbm, out_ref),
                (coupling_hbm, coupling_ref),
                (capacitance_hbm, scale_ref.at[0]),
                (saturation_hbm, scale_ref.at[1]),
                (steepness_hbm, scale_ref.at[2]),
                (junction_hbm, scale_ref.at[3]),
                (synthesis_hbm.at[me], synthesis_ref),
                (analysis_hbm.at[me], analysis_ref),
            ]
        )
    ]
    local[0].start()
    local[1].start()

    def round_chunk(chunk):
        load(chunk).wait()
        for inner in range(unit):
            block = chunk * unit + inner
            span = pl.ds(pl.multiple_of(block * LANES, LANES), LANES)
            for point in range(points):
                pool_ref[block, point * rows : (point + 1) * rows, :] = x_ref[
                    point, :, span
                ].astype(jnp.bfloat16)

    def send(chunk):
        for by in range(1, shares):
            exchange(chunk, by).start()

    round_chunk(0)
    for copy in local[2:]:
        copy.start()
    pl.semaphore_wait(barrier, greeted)

    def advance(chunk, carry):
        round_chunk(chunk)
        send(chunk - 1)
        return carry

    lax.fori_loop(1, chunks, advance, 0)
    local[0].wait()
    local[1].wait()
    for direction in range(len(OFFSETS)):
        for slot in range(slots):
            packed_ref[direction, slot] = pool_ref[list_ref[direction, slot, place]]
    send(chunks - 1)
    for direction, offset in enumerate(OFFSETS):

        @pl.when(on_mesh(place + offset))
        def _():
            halo(direction, place + offset).start()

    pool_ref[blocks + len(OFFSETS) * slots] = jnp.zeros(pool_ref.shape[1:], pool_ref.dtype)
    for copy in local[2:]:
        copy.wait()
    for direction, offset in enumerate(OFFSETS):
        first = blocks + direction * slots
        there = on_mesh(place - offset)

        @pl.when(there)
        def _():
            halo(direction, place - offset).wait_recv()
            for slot in range(slots):
                pool_ref[first + slot] = halo_ref[direction, slot]

        @pl.when(jnp.logical_not(there))
        def _():
            for slot in range(slots):
                pool_ref[first + slot] = jnp.zeros(pool_ref.shape[1:], pool_ref.dtype)

    row = me * rows + lax.broadcasted_iota(jnp.int32, (rows, LANES), 0)
    even = row % 2 == 0
    rate = (row // 2).astype(jnp.float32) * (2.0 / length)
    rate = jnp.where(even, rate, -rate)

    def couple(block, carry):
        gathered = jnp.concatenate([pool_ref[slot_ref[k, block]] for k in range(count)], axis=1)
        matrix = jnp.concatenate([coupling_ref[block, k] for k in range(count)], axis=1)
        coupled = lax.dot_general(
            gathered, matrix, (((1,), (1,)), ((), ())), preferred_element_type=jnp.float32
        )
        scaled = rate * scale_ref[0, pl.ds(block, 1), :]
        span = pl.ds(pl.multiple_of(block * LANES, LANES), LANES)
        for point in range(points):
            values = x_ref[point, :, span]
            other = jnp.where(even, pltpu.roll(values, rows - 1, 0), pltpu.roll(values, 1, 0))
            out_ref[point, :, span] = (
                coupled[point * rows : (point + 1) * rows]
                + scaled * other
                - out_ref[point, :, span]
            )
        return carry

    lax.fori_loop(0, blocks, couple, 0, unroll=unit)

    def nonlinear(chunk, carry):
        for by in range(1, shares):
            exchange(chunk, by).wait_recv()
        ids = [chunk * unit + inner for inner in range(unit)]
        scales = [widen(scale_ref, index, ids) for index in (1, 2, 3)]
        span = columns(chunk)
        for point in range(points):
            held = slice(point * rows, (point + 1) * rows)
            spectra = [jnp.concatenate([pool_ref[block, held, :] for block in ids], axis=1)]
            for by in range(1, shares):
                spectra.append(
                    jnp.concatenate([arrived_ref[by - 1, block, held, :] for block in ids], axis=1)
                )
            out_ref[point, :, span] += evaluate(
                spectra, synthesis_ref[...], analysis_ref[...], *scales
            )
        return carry

    lax.fori_loop(0, chunks - 1, nonlinear, 0)
    first = blocks - unit
    tail_ref[0] = pool_ref[first : first + unit]
    for by in range(1, shares):
        exchange(chunks - 1, by).wait_recv()
        tail_ref[by] = arrived_ref[by - 1, first : first + unit]

    def drain(chunk, carry):
        for by in range(1, shares):
            exchange(chunk, by).wait_send()
        return carry

    lax.fori_loop(0, chunks, drain, 0)
    for direction, offset in enumerate(OFFSETS):

        @pl.when(on_mesh(place + offset))
        def _():
            halo(direction, place + offset).wait_send()


def local_part(
    spectrum,
    source,
    coupling,
    capacitance,
    saturation,
    steepness,
    junction,
    halo_list,
    neighbour_slot,
):
    rows, points, nodes = spectrum.shape
    shares = lax.axis_size("harm")
    length = rows * shares
    blocks = nodes // LANES
    unit = 2 if blocks % 2 == 0 else 1
    chunks = blocks // unit
    slots, count = halo_list.shape[2], neighbour_slot.shape[1]
    directions = len(OFFSETS)
    pieces = 2 if rows % 16 == 0 else 1
    height = points * rows
    x = jnp.transpose(spectrum, (1, 0, 2))
    injected = jnp.transpose(source, (1, 0, 2))
    synthesis, analysis = (jnp.asarray(t) for t in fourier_tables(length, shares))
    scales = [v.reshape(blocks, LANES) for v in (capacitance, saturation, steepness, junction)]
    vmem = pl.BlockSpec(memory_space=pltpu.VMEM)
    hbm = pl.BlockSpec(memory_space=pltpu.HBM)
    bf16, f32 = jnp.bfloat16, jnp.float32
    held = pl.pallas_call(
        functools.partial(kernel, unit),
        in_specs=[hbm] * 11,
        out_specs=[vmem] * 5,
        out_shape=[
            pltpu.VMEM((points, rows, nodes), f32),
            pltpu.VMEM((shares, unit, height, LANES), bf16),
            pltpu.VMEM((length, 2 * length), bf16),
            pltpu.VMEM((rows, 2 * length), bf16),
            pltpu.VMEM((4, blocks, LANES), f32),
        ],
        scratch_shapes=[
            pltpu.SMEM((directions, slots, halo_list.shape[0]), jnp.int32),
            pltpu.SMEM((count, blocks), jnp.int32),
            pltpu.VMEM((points, rows, nodes), f32),
            pltpu.VMEM((blocks, count, LANES, LANES), bf16),
            pltpu.VMEM((blocks + directions * slots + 1, height, LANES), bf16),
            pltpu.VMEM((shares - 1, blocks, height, LANES), bf16),
            pltpu.VMEM((directions, slots, height, LANES), bf16),
            pltpu.VMEM((directions, slots, height, LANES), bf16),
            pltpu.SemaphoreType.DMA((chunks,)),
            pltpu.SemaphoreType.DMA((10,)),
            pltpu.SemaphoreType.DMA((shares - 1, chunks)),
            pltpu.SemaphoreType.DMA((shares - 1, chunks)),
            pltpu.SemaphoreType.DMA((directions,)),
            pltpu.SemaphoreType.DMA((directions,)),
        ],
        compiler_params=pltpu.CompilerParams(
            collective_id=0, has_side_effects=True, vmem_limit_bytes=VMEM_BYTES
        ),
        cost_estimate=pl.CostEstimate(
            flops=2 * height * nodes * (count * LANES + 3 * length),
            bytes_accessed=coupling.size * 2 + 3 * x.size * 4,
            transcendentals=0,
        ),
        name="residual",
    )(
        *[
            pltpu.with_memory_space_constraint(value, pltpu.HBM)
            for value in (
                jnp.transpose(halo_list, (1, 2, 0)),
                neighbour_slot.T,
                x,
                injected,
                coupling,
                synthesis,
                analysis,
                *scales,
            )
        ]
    )
    total = pl.pallas_call(
        functools.partial(finish_kernel, pieces),
        in_specs=[vmem] * 5,
        out_specs=hbm,
        out_shape=pltpu.HBM((points, rows, nodes), f32),
        scratch_shapes=[
            pltpu.VMEM((points, rows, unit * LANES), f32),
            pltpu.SemaphoreType.DMA((points * pieces + 1,)),
        ],
        compiler_params=pltpu.CompilerParams(vmem_limit_bytes=8 << 20),
        cost_estimate=pl.CostEstimate(
            flops=6 * height * unit * LANES * length, bytes_accessed=x.size * 4, transcendentals=0
        ),
        name="finish",
    )(*[pltpu.with_memory_space_constraint(value, pltpu.VMEM) for value in held])
    return jnp.transpose(total, (1, 0, 2))


def solution(mesh):
    in_specs = (
        P("harm", None, "node"),
        P("harm", None, "node"),
        P("node", None, None, None),
        P("node"),
        P("node"),
        P("node"),
        P("node"),
        P(),
        P("node", None),
    )
    return jax.shard_map(
        local_part, mesh=mesh, in_specs=in_specs, out_specs=P("harm", None, "node"), check_vma=False
    )
```

```python
import functools

import jax
import jax.numpy as jnp
import numpy as np
from jax import lax
from jax.experimental import pallas as pl
from jax.experimental.pallas import tpu as pltpu
from jax.sharding import PartitionSpec as P

LOG_TWO = 0.6931471805599453
OFFSETS = (-2, -1, 1, 2)
CUTS = (0, 2, 14, 26, 38, 44, 46, 48)
LANES = 128
VMEM_BYTES = 36 << 20
MESH = pl.DeviceIdType.MESH


def fourier_tables(length, shares):
    rows = length // shares
    sample = np.arange(length)[:, None]
    column = np.arange(length)[None, :]
    angle = 2.0 * np.pi / length * (column // 2 * sample % length)
    table = np.where(column % 2 == 1, np.sin(angle), np.cos(angle))
    table = np.where(column == 1, np.where(sample % 2 == 0, 1.0, -1.0), table)
    weights = np.where(np.arange(length) < 2, 1.0, 2.0) / length
    analysis = table.T * weights[:, None]
    pulsation = np.arange(length // 2)[:, None, None] / (length // 2)
    pairs = analysis.reshape(length // 2, 2, length)
    slope = np.concatenate([pulsation * pairs[:, 1:], -pulsation * pairs[:, :1]], axis=1)
    both = np.concatenate([analysis, slope.reshape(length, length)], axis=1)
    table = table.astype(np.float32)
    high = table.astype(jnp.bfloat16)
    low = (table - high.astype(np.float32)).astype(jnp.bfloat16)
    order = [
        np.concatenate([np.arange(rows) + (me - by) % shares * rows for by in range(shares)])
        for me in range(shares)
    ]
    synthesis = np.stack([np.concatenate([high[:, o], low[:, o]], axis=1) for o in order])
    return synthesis, both.astype(jnp.bfloat16).reshape(shares, rows, 2 * length)


def evaluate(spectra, synthesis, analysis, saturation, steepness, junction):
    stacked = jnp.concatenate(spectra + spectra, axis=0)
    voltage = jnp.dot(synthesis, stacked, preferred_element_type=jnp.float32)
    drive = steepness * voltage
    softplus = jnp.maximum(drive, 0.0) + jnp.log(1.0 + jnp.exp(-jnp.abs(drive)))
    current = (saturation * (softplus - LOG_TWO)).astype(jnp.bfloat16)
    charge = (junction * voltage * lax.rsqrt(1.0 + voltage * voltage)).astype(jnp.bfloat16)
    samples = jnp.concatenate([current, charge], axis=0)
    return jnp.dot(analysis, samples, preferred_element_type=jnp.float32)


def widen(scale_ref, index, blocks):
    parts = [scale_ref[index, pl.ds(block, 1), :] for block in blocks]
    return jnp.concatenate(parts, axis=1)


def finish_kernel(pieces, total_ref, tail_ref, synthesis_ref, analysis_ref, scale_ref, out_hbm, last_ref, sem):
    points, rows, nodes = total_ref.shape
    shares, unit = tail_ref.shape[:2]
    blocks = nodes // LANES
    done = nodes - unit * LANES
    copies = []
    for point in range(points):
        for piece in range(pieces):
            part = (point, slice(piece * rows // pieces, (piece + 1) * rows // pieces), slice(0, done))
            copies.append(
                pltpu.make_async_copy(
                    total_ref.at[part], out_hbm.at[part], sem.at[point * pieces + piece]
                )
            )
    for copy in copies:
        copy.start()
    ids = range(blocks - unit, blocks)
    scales = [widen(scale_ref, index, ids) for index in (1, 2, 3)]
    for point in range(points):
        held = slice(point * rows, (point + 1) * rows)
        spectra = [
            jnp.concatenate([tail_ref[share, inner, held, :] for inner in range(unit)], axis=1)
            for share in range(shares)
        ]
        last_ref[point] = total_ref[point, :, done:] + evaluate(
            spectra, synthesis_ref[...], analysis_ref[...], *scales
        )
    copy = pltpu.make_async_copy(last_ref, out_hbm.at[:, :, done:], sem.at[points * pieces])
    copy.start()
    for each in copies + [copy]:
        each.wait()


def kernel(
    unit,
    bounds,
    list_hbm,
    slot_hbm,
    x_hbm,
    source_hbm,
    coupling_hbm,
    synthesis_hbm,
    analysis_hbm,
    capacitance_hbm,
    saturation_hbm,
    steepness_hbm,
    junction_hbm,
    out_ref,
    tail_ref,
    synthesis_ref,
    analysis_ref,
    scale_ref,
    list_ref,
    slot_ref,
    x_ref,
    coupling_ref,
    pool_ref,
    arrived_ref,
    packed_ref,
    halo_ref,
    x_sem,
    local_sem,
    send_sem,
    recv_sem,
    halo_send_sem,
    halo_recv_sem,
):
    points, rows, nodes = x_ref.shape
    blocks = nodes // LANES
    chunks = len(bounds) - 1
    count, slots = coupling_ref.shape[1], list_ref.shape[1]
    shares, devices = lax.axis_size("harm"), lax.axis_size("node")
    me, place = lax.axis_index("harm"), lax.axis_index("node")
    length = rows * shares

    def on_mesh(device):
        return jnp.logical_and(device >= 0, device < devices)

    def load(chunk):
        span = slice(bounds[chunk] * LANES, bounds[chunk + 1] * LANES)
        return pltpu.make_async_copy(
            x_hbm.at[:, :, span], x_ref.at[:, :, span], x_sem.at[chunk]
        )

    def exchange(low, high, by, recv):
        return pltpu.make_async_remote_copy(
            src_ref=pool_ref.at[low:high],
            dst_ref=arrived_ref.at[by - 1, low:high],
            send_sem=send_sem.at[by - 1],
            recv_sem=recv_sem.at[by - 1, recv],
            device_id={"harm": lax.rem(me + by, shares)},
            device_id_type=MESH,
        )

    def part(chunk, by):
        return exchange(bounds[chunk], bounds[chunk + 1], by, chunk)

    def halo(direction, device):
        return pltpu.make_async_remote_copy(
            src_ref=packed_ref.at[direction],
            dst_ref=halo_ref.at[direction],
            send_sem=halo_send_sem.at[direction],
            recv_sem=halo_recv_sem.at[direction],
            device_id={"node": device},
            device_id_type=MESH,
        )

    barrier = pltpu.get_barrier_semaphore()
    for by in range(1, shares):
        pl.semaphore_signal(
            barrier, inc=1, device_id={"harm": lax.rem(me + by, shares)}, device_id_type=MESH
        )
    greeted = shares - 1
    for offset in OFFSETS:
        there = on_mesh(place + offset)
        greeted = greeted + there.astype(jnp.int32)

        @pl.when(there)
        def _():
            pl.semaphore_signal(
                barrier, inc=1, device_id={"node": place + offset}, device_id_type=MESH
            )

    for chunk in range(chunks):
        load(chunk).start()
    tables = [
        pltpu.make_async_copy(source, target, local_sem.at[i])
        for i, (source, target) in enumerate([(list_hbm, list_ref), (slot_hbm, slot_ref)])
    ]
    large = [
        pltpu.make_async_copy(source, target, local_sem.at[i + 2])
        for i, (source, target) in enumerate(
            [
                (source_hbm, out_ref),
                (coupling_hbm, coupling_ref),
                (synthesis_hbm.at[me], synthesis_ref),
                (analysis_hbm.at[me], analysis_ref),
            ]
        )
    ]
    scales = [
        pltpu.make_async_copy(source, scale_ref.at[i], local_sem.at[6])
        for i, source in enumerate([capacitance_hbm, saturation_hbm, steepness_hbm, junction_hbm])
    ]
    for copy in tables:
        copy.start()

    def round_block(block, carry):
        span = pl.ds(pl.multiple_of(block * LANES, LANES), LANES)
        for point in range(points):
            pool_ref[block, point * rows : (point + 1) * rows, :] = x_ref[point, :, span].astype(
                jnp.bfloat16
            )
        return carry

    def round_chunk(chunk):
        load(chunk).wait()
        lax.fori_loop(bounds[chunk], bounds[chunk + 1], round_block, 0, unroll=unit)

    def send(chunk):
        for by in range(1, shares):
            part(chunk, by).start()

    round_chunk(0)
    for copy in large + scales:
        copy.start()
    pl.semaphore_wait(barrier, greeted)
    for chunk in range(1, chunks):
        round_chunk(chunk)
        send(chunk - 1)
    for copy in tables:
        copy.wait()
    for direction in range(len(OFFSETS)):
        for slot in range(slots):
            packed_ref[direction, slot] = pool_ref[list_ref[direction, slot, place]]
    send(chunks - 1)
    for direction, offset in enumerate(OFFSETS):

        @pl.when(on_mesh(place + offset))
        def _():
            halo(direction, place + offset).start()

    pool_ref[blocks + len(OFFSETS) * slots] = jnp.zeros(pool_ref.shape[1:], pool_ref.dtype)
    for copy in large:
        copy.wait()
    pltpu.make_async_copy(scale_ref, scale_ref, local_sem.at[6]).wait()
    for direction, offset in enumerate(OFFSETS):
        first = blocks + direction * slots
        there = on_mesh(place - offset)

        @pl.when(there)
        def _():
            halo(direction, place - offset).wait_recv()
            for slot in range(slots):
                pool_ref[first + slot] = halo_ref[direction, slot]

        @pl.when(jnp.logical_not(there))
        def _():
            for slot in range(slots):
                pool_ref[first + slot] = jnp.zeros(pool_ref.shape[1:], pool_ref.dtype)

    row = me * rows + lax.broadcasted_iota(jnp.int32, (rows, LANES), 0)
    even = row % 2 == 0
    rate = (row // 2).astype(jnp.float32) * (2.0 / length)
    rate = jnp.where(even, rate, -rate)

    def couple(block, carry):
        gathered = jnp.concatenate([pool_ref[slot_ref[k, block]] for k in range(count)], axis=1)
        matrix = jnp.concatenate([coupling_ref[block, k] for k in range(count)], axis=1)
        coupled = lax.dot_general(
            gathered, matrix, (((1,), (1,)), ((), ())), preferred_element_type=jnp.float32
        )
        scaled = rate * scale_ref[0, pl.ds(block, 1), :]
        span = pl.ds(pl.multiple_of(block * LANES, LANES), LANES)
        for point in range(points):
            values = x_ref[point, :, span]
            other = jnp.where(even, pltpu.roll(values, rows - 1, 0), pltpu.roll(values, 1, 0))
            out_ref[point, :, span] = (
                coupled[point * rows : (point + 1) * rows]
                + scaled * other
                - out_ref[point, :, span]
            )
        return carry

    lax.fori_loop(0, blocks, couple, 0, unroll=unit)

    def nonlinear(group, carry):
        ids = [group * unit + inner for inner in range(unit)]
        factors = [widen(scale_ref, index, ids) for index in (1, 2, 3)]
        span = pl.ds(pl.multiple_of(group * unit * LANES, unit * LANES), unit * LANES)
        for point in range(points):
            held = slice(point * rows, (point + 1) * rows)
            spectra = [jnp.concatenate([pool_ref[block, held, :] for block in ids], axis=1)]
            for by in range(1, shares):
                spectra.append(
                    jnp.concatenate([arrived_ref[by - 1, block, held, :] for block in ids], axis=1)
                )
            out_ref[point, :, span] += evaluate(
                spectra, synthesis_ref[...], analysis_ref[...], *factors
            )
        return carry

    for chunk in range(chunks - 1):
        for by in range(1, shares):
            part(chunk, by).wait_recv()
        lax.fori_loop(bounds[chunk] // unit, bounds[chunk + 1] // unit, nonlinear, 0)
    first = bounds[chunks - 1]
    tail_ref[0] = pool_ref[first:blocks]
    for by in range(1, shares):
        part(chunks - 1, by).wait_recv()
        tail_ref[by] = arrived_ref[by - 1, first:blocks]

    for by in range(1, shares):
        exchange(0, blocks, by, 0).wait_send()
    for direction, offset in enumerate(OFFSETS):

        @pl.when(on_mesh(place + offset))
        def _():
            halo(direction, place + offset).wait_send()


def local_part(
    spectrum,
    source,
    coupling,
    capacitance,
    saturation,
    steepness,
    junction,
    halo_list,
    neighbour_slot,
):
    rows, points, nodes = spectrum.shape
    shares = lax.axis_size("harm")
    length = rows * shares
    blocks = nodes // LANES
    unit = 2 if blocks % 2 == 0 else 1
    bounds = sorted({cut * blocks // CUTS[-1] // unit * unit for cut in CUTS})
    chunks, last = len(bounds) - 1, blocks - bounds[-2]
    slots, count = halo_list.shape[2], neighbour_slot.shape[1]
    directions = len(OFFSETS)
    pieces = 1
    height = points * rows
    x = jnp.transpose(spectrum, (1, 0, 2))
    injected = jnp.transpose(source, (1, 0, 2))
    synthesis, analysis = (jnp.asarray(t) for t in fourier_tables(length, shares))
    scales = [v.reshape(blocks, LANES) for v in (capacitance, saturation, steepness, junction)]
    vmem = pl.BlockSpec(memory_space=pltpu.VMEM)
    hbm = pl.BlockSpec(memory_space=pltpu.HBM)
    bf16, f32 = jnp.bfloat16, jnp.float32
    held = pl.pallas_call(
        functools.partial(kernel, unit, bounds),
        in_specs=[hbm] * 11,
        out_specs=[vmem] * 5,
        out_shape=[
            pltpu.VMEM((points, rows, nodes), f32),
            pltpu.VMEM((shares, last, height, LANES), bf16),
            pltpu.VMEM((length, 2 * length), bf16),
            pltpu.VMEM((rows, 2 * length), bf16),
            pltpu.VMEM((4, blocks, LANES), f32),
        ],
        scratch_shapes=[
            pltpu.SMEM((directions, slots, halo_list.shape[0]), jnp.int32),
            pltpu.SMEM((count, blocks), jnp.int32),
            pltpu.VMEM((points, rows, nodes), f32),
            pltpu.VMEM((blocks, count, LANES, LANES), bf16),
            pltpu.VMEM((blocks + directions * slots + 1, height, LANES), bf16),
            pltpu.VMEM((shares - 1, blocks, height, LANES), bf16),
            pltpu.VMEM((directions, slots, height, LANES), bf16),
            pltpu.VMEM((directions, slots, height, LANES), bf16),
            pltpu.SemaphoreType.DMA((chunks,)),
            pltpu.SemaphoreType.DMA((7,)),
            pltpu.SemaphoreType.DMA((shares - 1,)),
            pltpu.SemaphoreType.DMA((shares - 1, chunks)),
            pltpu.SemaphoreType.DMA((directions,)),
            pltpu.SemaphoreType.DMA((directions,)),
        ],
        compiler_params=pltpu.CompilerParams(
            collective_id=0, has_side_effects=True, vmem_limit_bytes=VMEM_BYTES
        ),
        cost_estimate=pl.CostEstimate(
            flops=2 * height * nodes * (count * LANES + 3 * length),
            bytes_accessed=coupling.size * 2 + 3 * x.size * 4,
            transcendentals=0,
        ),
        name="residual",
    )(
        *[
            pltpu.with_memory_space_constraint(value, pltpu.HBM)
            for value in (
                jnp.transpose(halo_list, (1, 2, 0)),
                neighbour_slot.T,
                x,
                injected,
                coupling,
                synthesis,
                analysis,
                *scales,
            )
        ]
    )
    total = pl.pallas_call(
        functools.partial(finish_kernel, pieces),
        in_specs=[vmem] * 5,
        out_specs=hbm,
        out_shape=pltpu.HBM((points, rows, nodes), f32),
        scratch_shapes=[
            pltpu.VMEM((points, rows, last * LANES), f32),
            pltpu.SemaphoreType.DMA((points * pieces + 1,)),
        ],
        compiler_params=pltpu.CompilerParams(vmem_limit_bytes=8 << 20),
        cost_estimate=pl.CostEstimate(
            flops=6 * height * last * LANES * length, bytes_accessed=x.size * 4, transcendentals=0
        ),
        name="finish",
    )(*[pltpu.with_memory_space_constraint(value, pltpu.VMEM) for value in held])
    return jnp.transpose(total, (1, 0, 2))


def solution(mesh):
    in_specs = (
        P("harm", None, "node"),
        P("harm", None, "node"),
        P("node", None, None, None),
        P("node"),
        P("node"),
        P("node"),
        P("node"),
        P(),
        P("node", None),
    )
    return jax.shard_map(
        local_part, mesh=mesh, in_specs=in_specs, out_specs=P("harm", None, "node"), check_vma=False
    )
```

```python
import functools

import jax
import jax.numpy as jnp
import numpy as np
from jax import lax
from jax.experimental import pallas as pl
from jax.experimental.pallas import tpu as pltpu
from jax.sharding import PartitionSpec as P

LOG_TWO = 0.6931471805599453
OFFSETS = (-2, -1, 1, 2)
CUTS = (0, 2, 14, 26, 38, 44, 46, 48)
LANES = 128
VMEM_BYTES = 36 << 20
MESH = pl.DeviceIdType.MESH


def fourier_tables(length, shares):
    rows = length // shares
    sample = np.arange(length)[:, None]
    column = np.arange(length)[None, :]
    angle = 2.0 * np.pi / length * (column // 2 * sample % length)
    table = np.where(column % 2 == 1, np.sin(angle), np.cos(angle))
    table = np.where(column == 1, np.where(sample % 2 == 0, 1.0, -1.0), table)
    weights = np.where(np.arange(length) < 2, 1.0, 2.0) / length
    analysis = table.T * weights[:, None]
    pulsation = np.arange(length // 2)[:, None, None] / (length // 2)
    pairs = analysis.reshape(length // 2, 2, length)
    slope = np.concatenate([pulsation * pairs[:, 1:], -pulsation * pairs[:, :1]], axis=1)
    both = np.concatenate([analysis, slope.reshape(length, length)], axis=1)
    table = table.astype(np.float32)
    high = table.astype(jnp.bfloat16)
    low = (table - high.astype(np.float32)).astype(jnp.bfloat16)
    order = [
        np.concatenate([np.arange(rows) + (me - by) % shares * rows for by in range(shares)])
        for me in range(shares)
    ]
    synthesis = np.stack([np.concatenate([high[:, o], low[:, o]], axis=1) for o in order])
    return synthesis, both.astype(jnp.bfloat16).reshape(shares, rows, 2 * length)


def evaluate(spectra, synthesis, analysis, saturation, steepness, junction):
    stacked = jnp.concatenate(spectra + spectra, axis=0)
    voltage = jnp.dot(synthesis, stacked, preferred_element_type=jnp.float32)
    drive = steepness * voltage
    softplus = jnp.maximum(drive, 0.0) + jnp.log(1.0 + jnp.exp(-jnp.abs(drive)))
    current = (saturation * (softplus - LOG_TWO)).astype(jnp.bfloat16)
    charge = (junction * voltage * lax.rsqrt(1.0 + voltage * voltage)).astype(jnp.bfloat16)
    samples = jnp.concatenate([current, charge], axis=0)
    return jnp.dot(analysis, samples, preferred_element_type=jnp.float32)


def widen(scale_ref, index, blocks):
    parts = [scale_ref[index, pl.ds(block, 1), :] for block in blocks]
    return jnp.concatenate(parts, axis=1)


def finish_kernel(pieces, total_ref, tail_ref, synthesis_ref, analysis_ref, scale_ref, out_hbm, last_ref, sem):
    points, rows, nodes = total_ref.shape
    shares, unit = tail_ref.shape[:2]
    blocks = nodes // LANES
    done = nodes - unit * LANES
    copies = []
    for point in range(points):
        for piece in range(pieces):
            part = (point, slice(piece * rows // pieces, (piece + 1) * rows // pieces), slice(0, done))
            copies.append(
                pltpu.make_async_copy(
                    total_ref.at[part], out_hbm.at[part], sem.at[point * pieces + piece]
                )
            )
    for copy in copies:
        copy.start()
    ids = range(blocks - unit, blocks)
    scales = [widen(scale_ref, index, ids) for index in (1, 2, 3)]
    for point in range(points):
        held = slice(point * rows, (point + 1) * rows)
        spectra = [
            jnp.concatenate([tail_ref[share, inner, held, :] for inner in range(unit)], axis=1)
            for share in range(shares)
        ]
        last_ref[point] = total_ref[point, :, done:] + evaluate(
            spectra, synthesis_ref[...], analysis_ref[...], *scales
        )
    copy = pltpu.make_async_copy(last_ref, out_hbm.at[:, :, done:], sem.at[points * pieces])
    copy.start()
    for each in copies + [copy]:
        each.wait()


def kernel(
    unit,
    bounds,
    list_hbm,
    slot_hbm,
    x_hbm,
    source_hbm,
    coupling_hbm,
    synthesis_hbm,
    analysis_hbm,
    capacitance_hbm,
    saturation_hbm,
    steepness_hbm,
    junction_hbm,
    out_ref,
    tail_ref,
    synthesis_ref,
    analysis_ref,
    scale_ref,
    list_ref,
    slot_ref,
    x_ref,
    coupling_ref,
    pool_ref,
    arrived_ref,
    packed_ref,
    halo_ref,
    x_sem,
    local_sem,
    send_sem,
    recv_sem,
    halo_send_sem,
    halo_recv_sem,
    ready_sem,
    start_sem,
    group_sem,
    halo_sem,
):
    points, rows, nodes = x_ref.shape
    blocks = nodes // LANES
    chunks = len(bounds) - 1
    count, slots = coupling_ref.shape[1], list_ref.shape[1]
    shares, devices = lax.axis_size("harm"), lax.axis_size("node")
    me, place = lax.axis_index("harm"), lax.axis_index("node")
    length = rows * shares

    def on_mesh(device):
        return jnp.logical_and(device >= 0, device < devices)

    def load(chunk):
        span = slice(bounds[chunk] * LANES, bounds[chunk + 1] * LANES)
        return pltpu.make_async_copy(
            x_hbm.at[:, :, span], x_ref.at[:, :, span], x_sem.at[chunk]
        )

    def exchange(low, high, by, recv):
        return pltpu.make_async_remote_copy(
            src_ref=pool_ref.at[low:high],
            dst_ref=arrived_ref.at[by - 1, low:high],
            send_sem=send_sem.at[by - 1],
            recv_sem=recv_sem.at[by - 1, recv],
            device_id={"harm": lax.rem(me + by, shares)},
            device_id_type=MESH,
        )

    def part(chunk, by):
        return exchange(bounds[chunk], bounds[chunk + 1], by, chunk)

    def halo(direction, device):
        return pltpu.make_async_remote_copy(
            src_ref=packed_ref.at[direction],
            dst_ref=halo_ref.at[direction],
            send_sem=halo_send_sem.at[direction],
            recv_sem=halo_recv_sem.at[direction],
            device_id={"node": device},
            device_id_type=MESH,
        )

    root = me == 0
    member = jnp.logical_not(root)
    group = [{"harm": other} for other in range(1, shares)]
    barrier = pltpu.get_barrier_semaphore()
    load(0).start()

    def signal(semaphore, device):
        pl.semaphore_signal(semaphore, inc=1, device_id=device, device_id_type=MESH)

    @pl.when(root)
    def _():
        for other in group:
            signal(barrier, other)

    def greet(semaphore):
        for offset in OFFSETS:

            @pl.when(jnp.logical_and(root, on_mesh(place + offset)))
            def _():
                signal(semaphore, {"node": place + offset})

    greet(barrier)
    greeted = sum(on_mesh(place + offset).astype(jnp.int32) for offset in OFFSETS)
    for chunk in range(1, chunks):
        load(chunk).start()
    tables = [
        pltpu.make_async_copy(source, target, local_sem.at[i])
        for i, (source, target) in enumerate([(list_hbm, list_ref), (slot_hbm, slot_ref)])
    ]
    large = [
        pltpu.make_async_copy(source, target, local_sem.at[i + 2])
        for i, (source, target) in enumerate(
            [
                (source_hbm, out_ref),
                (coupling_hbm, coupling_ref),
                (synthesis_hbm.at[me], synthesis_ref),
                (analysis_hbm.at[me], analysis_ref),
            ]
        )
    ]
    scales = [
        pltpu.make_async_copy(source, scale_ref.at[i], local_sem.at[6])
        for i, source in enumerate([capacitance_hbm, saturation_hbm, steepness_hbm, junction_hbm])
    ]
    for copy in tables:
        copy.start()

    def round_block(block, carry):
        span = pl.ds(pl.multiple_of(block * LANES, LANES), LANES)
        for point in range(points):
            pool_ref[block, point * rows : (point + 1) * rows, :] = x_ref[point, :, span].astype(
                jnp.bfloat16
            )
        return carry

    def round_chunk(chunk):
        load(chunk).wait()
        lax.fori_loop(bounds[chunk], bounds[chunk + 1], round_block, 0, unroll=unit)

    def send(chunk):
        for by in range(1, shares):
            part(chunk, by).start()

    @pl.when(member)
    def _():
        pl.semaphore_wait(barrier, 1)
        signal(ready_sem, {"harm": 0})

    round_chunk(0)
    for copy in large + scales:
        copy.start()

    @pl.when(root)
    def _():
        pl.semaphore_wait(barrier, greeted)
        pl.semaphore_wait(ready_sem, shares - 1)
        if shares > 2:
            for other in group:
                signal(start_sem, other)

    if shares > 2:

        @pl.when(member)
        def _():
            pl.semaphore_wait(start_sem, 1)

    for chunk in range(1, chunks):
        round_chunk(chunk)
        send(chunk - 1)
    for copy in tables:
        copy.wait()
    for direction in range(len(OFFSETS)):
        for slot in range(slots):
            packed_ref[direction, slot] = pool_ref[list_ref[direction, slot, place]]
    send(chunks - 1)
    greet(group_sem)

    @pl.when(root)
    def _():
        pl.semaphore_wait(group_sem, greeted)
        for other in group:
            signal(halo_sem, other)

    @pl.when(member)
    def _():
        pl.semaphore_wait(halo_sem, 1)

    for direction, offset in enumerate(OFFSETS):

        @pl.when(on_mesh(place + offset))
        def _():
            halo(direction, place + offset).start()

    pool_ref[blocks + len(OFFSETS) * slots] = jnp.zeros(pool_ref.shape[1:], pool_ref.dtype)
    for copy in large:
        copy.wait()
    pltpu.make_async_copy(scale_ref, scale_ref, local_sem.at[6]).wait()
    for direction, offset in enumerate(OFFSETS):
        first = blocks + direction * slots
        there = on_mesh(place - offset)

        @pl.when(there)
        def _():
            halo(direction, place - offset).wait_recv()
            for slot in range(slots):
                pool_ref[first + slot] = halo_ref[direction, slot]

        @pl.when(jnp.logical_not(there))
        def _():
            for slot in range(slots):
                pool_ref[first + slot] = jnp.zeros(pool_ref.shape[1:], pool_ref.dtype)

    row = me * rows + lax.broadcasted_iota(jnp.int32, (rows, LANES), 0)
    even = row % 2 == 0
    rate = (row // 2).astype(jnp.float32) * (2.0 / length)
    rate = jnp.where(even, rate, -rate)

    def couple(block, carry):
        gathered = jnp.concatenate([pool_ref[slot_ref[k, block]] for k in range(count)], axis=1)
        matrix = jnp.concatenate([coupling_ref[block, k] for k in range(count)], axis=1)
        coupled = lax.dot_general(
            gathered, matrix, (((1,), (1,)), ((), ())), preferred_element_type=jnp.float32
        )
        scaled = rate * scale_ref[0, pl.ds(block, 1), :]
        span = pl.ds(pl.multiple_of(block * LANES, LANES), LANES)
        for point in range(points):
            values = x_ref[point, :, span]
            other = jnp.where(even, pltpu.roll(values, rows - 1, 0), pltpu.roll(values, 1, 0))
            out_ref[point, :, span] = (
                coupled[point * rows : (point + 1) * rows]
                + scaled * other
                - out_ref[point, :, span]
            )
        return carry

    lax.fori_loop(0, blocks, couple, 0, unroll=unit)

    def nonlinear(group, carry):
        ids = [group * unit + inner for inner in range(unit)]
        factors = [widen(scale_ref, index, ids) for index in (1, 2, 3)]
        span = pl.ds(pl.multiple_of(group * unit * LANES, unit * LANES), unit * LANES)
        for point in range(points):
            held = slice(point * rows, (point + 1) * rows)
            spectra = [jnp.concatenate([pool_ref[block, held, :] for block in ids], axis=1)]
            for by in range(1, shares):
                spectra.append(
                    jnp.concatenate([arrived_ref[by - 1, block, held, :] for block in ids], axis=1)
                )
            out_ref[point, :, span] += evaluate(
                spectra, synthesis_ref[...], analysis_ref[...], *factors
            )
        return carry

    for chunk in range(chunks - 1):
        for by in range(1, shares):
            part(chunk, by).wait_recv()
        lax.fori_loop(bounds[chunk] // unit, bounds[chunk + 1] // unit, nonlinear, 0)
    first = bounds[chunks - 1]
    tail_ref[0] = pool_ref[first:blocks]
    for by in range(1, shares):
        part(chunks - 1, by).wait_recv()
        tail_ref[by] = arrived_ref[by - 1, first:blocks]

    for by in range(1, shares):
        exchange(0, blocks, by, 0).wait_send()
    for direction, offset in enumerate(OFFSETS):

        @pl.when(on_mesh(place + offset))
        def _():
            halo(direction, place + offset).wait_send()


def local_part(
    spectrum,
    source,
    coupling,
    capacitance,
    saturation,
    steepness,
    junction,
    halo_list,
    neighbour_slot,
):
    rows, points, nodes = spectrum.shape
    shares = lax.axis_size("harm")
    length = rows * shares
    blocks = nodes // LANES
    unit = 2 if blocks % 2 == 0 else 1
    bounds = sorted({cut * blocks // CUTS[-1] // unit * unit for cut in CUTS})
    chunks, last = len(bounds) - 1, blocks - bounds[-2]
    slots, count = halo_list.shape[2], neighbour_slot.shape[1]
    directions = len(OFFSETS)
    pieces = 1
    height = points * rows
    x = jnp.transpose(spectrum, (1, 0, 2))
    injected = jnp.transpose(source, (1, 0, 2))
    synthesis, analysis = (jnp.asarray(t) for t in fourier_tables(length, shares))
    scales = [v.reshape(blocks, LANES) for v in (capacitance, saturation, steepness, junction)]
    vmem = pl.BlockSpec(memory_space=pltpu.VMEM)
    hbm = pl.BlockSpec(memory_space=pltpu.HBM)
    bf16, f32 = jnp.bfloat16, jnp.float32
    held = pl.pallas_call(
        functools.partial(kernel, unit, bounds),
        in_specs=[hbm] * 11,
        out_specs=[vmem] * 5,
        out_shape=[
            pltpu.VMEM((points, rows, nodes), f32),
            pltpu.VMEM((shares, last, height, LANES), bf16),
            pltpu.VMEM((length, 2 * length), bf16),
            pltpu.VMEM((rows, 2 * length), bf16),
            pltpu.VMEM((4, blocks, LANES), f32),
        ],
        scratch_shapes=[
            pltpu.SMEM((directions, slots, halo_list.shape[0]), jnp.int32),
            pltpu.SMEM((count, blocks), jnp.int32),
            pltpu.VMEM((points, rows, nodes), f32),
            pltpu.VMEM((blocks, count, LANES, LANES), bf16),
            pltpu.VMEM((blocks + directions * slots + 1, height, LANES), bf16),
            pltpu.VMEM((shares - 1, blocks, height, LANES), bf16),
            pltpu.VMEM((directions, slots, height, LANES), bf16),
            pltpu.VMEM((directions, slots, height, LANES), bf16),
            pltpu.SemaphoreType.DMA((chunks,)),
            pltpu.SemaphoreType.DMA((7,)),
            pltpu.SemaphoreType.DMA((shares - 1,)),
            pltpu.SemaphoreType.DMA((shares - 1, chunks)),
            pltpu.SemaphoreType.DMA((directions,)),
            pltpu.SemaphoreType.DMA((directions,)),
        ]
        + [pltpu.SemaphoreType.REGULAR] * 4,
        compiler_params=pltpu.CompilerParams(
            collective_id=0, has_side_effects=True, vmem_limit_bytes=VMEM_BYTES
        ),
        cost_estimate=pl.CostEstimate(
            flops=2 * height * nodes * (count * LANES + 3 * length),
            bytes_accessed=coupling.size * 2 + 3 * x.size * 4,
            transcendentals=0,
        ),
        name="residual",
    )(
        *[
            pltpu.with_memory_space_constraint(value, pltpu.HBM)
            for value in (
                jnp.transpose(halo_list, (1, 2, 0)),
                neighbour_slot.T,
                x,
                injected,
                coupling,
                synthesis,
                analysis,
                *scales,
            )
        ]
    )
    total = pl.pallas_call(
        functools.partial(finish_kernel, pieces),
        in_specs=[vmem] * 5,
        out_specs=hbm,
        out_shape=pltpu.HBM((points, rows, nodes), f32),
        scratch_shapes=[
            pltpu.VMEM((points, rows, last * LANES), f32),
            pltpu.SemaphoreType.DMA((points * pieces + 1,)),
        ],
        compiler_params=pltpu.CompilerParams(vmem_limit_bytes=8 << 20),
        cost_estimate=pl.CostEstimate(
            flops=6 * height * last * LANES * length, bytes_accessed=x.size * 4, transcendentals=0
        ),
        name="finish",
    )(*[pltpu.with_memory_space_constraint(value, pltpu.VMEM) for value in held])
    return jnp.transpose(total, (1, 0, 2))


def solution(mesh):
    in_specs = (
        P("harm", None, "node"),
        P("harm", None, "node"),
        P("node", None, None, None),
        P("node"),
        P("node"),
        P("node"),
        P("node"),
        P(),
        P("node", None),
    )
    return jax.shard_map(
        local_part, mesh=mesh, in_specs=in_specs, out_specs=P("harm", None, "node"), check_vma=False
    )
```

```python
import functools

import jax
import jax.numpy as jnp
import numpy as np
from jax import lax
from jax.experimental import pallas as pl
from jax.experimental.pallas import tpu as pltpu
from jax.sharding import PartitionSpec as P

LOG_TWO = 0.6931471805599453
OFFSETS = (-2, -1, 1, 2)
CUTS = (0, 2, 4, 14, 26, 38, 44, 46, 48)
LANES = 128
VMEM_BYTES = 36 << 20
MESH = pl.DeviceIdType.MESH


def fourier_tables(length, shares):
    rows = length // shares
    sample = np.arange(length)[:, None]
    column = np.arange(length)[None, :]
    angle = 2.0 * np.pi / length * (column // 2 * sample % length)
    table = np.where(column % 2 == 1, np.sin(angle), np.cos(angle))
    table = np.where(column == 1, np.where(sample % 2 == 0, 1.0, -1.0), table)
    weights = np.where(np.arange(length) < 2, 1.0, 2.0) / length
    analysis = table.T * weights[:, None]
    pulsation = np.arange(length // 2)[:, None, None] / (length // 2)
    pairs = analysis.reshape(length // 2, 2, length)
    slope = np.concatenate([pulsation * pairs[:, 1:], -pulsation * pairs[:, :1]], axis=1)
    both = np.concatenate([analysis, slope.reshape(length, length)], axis=1)
    table = table.astype(np.float32)
    high = table.astype(jnp.bfloat16)
    low = (table - high.astype(np.float32)).astype(jnp.bfloat16)
    order = [
        np.concatenate([np.arange(rows) + (me - by) % shares * rows for by in range(shares)])
        for me in range(shares)
    ]
    synthesis = np.stack([np.concatenate([high[:, o], low[:, o]], axis=1) for o in order])
    return synthesis, both.astype(jnp.bfloat16).reshape(shares, rows, 2 * length)


def evaluate(spectra, synthesis, analysis, saturation, steepness, junction):
    stacked = jnp.concatenate(spectra + spectra, axis=0)
    voltage = jnp.dot(synthesis, stacked, preferred_element_type=jnp.float32)
    drive = steepness * voltage
    softplus = jnp.maximum(drive, 0.0) + jnp.log(1.0 + jnp.exp(-jnp.abs(drive)))
    current = (saturation * (softplus - LOG_TWO)).astype(jnp.bfloat16)
    charge = (junction * voltage * lax.rsqrt(1.0 + voltage * voltage)).astype(jnp.bfloat16)
    samples = jnp.concatenate([current, charge], axis=0)
    return jnp.dot(analysis, samples, preferred_element_type=jnp.float32)


def widen(scale_ref, index, blocks):
    parts = [scale_ref[index, pl.ds(block, 1), :] for block in blocks]
    return jnp.concatenate(parts, axis=1)


def finish_kernel(total_ref, tail_ref, synthesis_ref, analysis_ref, scale_ref, out_hbm, last_ref, sem):
    points, rows, nodes = total_ref.shape
    shares, unit = tail_ref.shape[:2]
    blocks = nodes // LANES
    done = nodes - unit * LANES
    bulk = pltpu.make_async_copy(
        total_ref.at[:, :, :done], out_hbm.at[:, :, :done], sem.at[0]
    )
    bulk.start()
    ids = range(blocks - unit, blocks)
    scales = [widen(scale_ref, index, ids) for index in (1, 2, 3)]
    for point in range(points):
        held = slice(point * rows, (point + 1) * rows)
        spectra = [
            jnp.concatenate([tail_ref[share, inner, held, :] for inner in range(unit)], axis=1)
            for share in range(shares)
        ]
        last_ref[point] = total_ref[point, :, done:] + evaluate(
            spectra, synthesis_ref[...], analysis_ref[...], *scales
        )
    copy = pltpu.make_async_copy(last_ref, out_hbm.at[:, :, done:], sem.at[1])
    copy.start()
    bulk.wait()
    copy.wait()


def kernel(
    unit,
    bounds,
    list_hbm,
    slot_hbm,
    x_hbm,
    source_hbm,
    coupling_hbm,
    synthesis_hbm,
    analysis_hbm,
    capacitance_hbm,
    saturation_hbm,
    steepness_hbm,
    junction_hbm,
    out_ref,
    tail_ref,
    synthesis_ref,
    analysis_ref,
    scale_ref,
    list_ref,
    slot_ref,
    x_ref,
    coupling_ref,
    pool_ref,
    arrived_ref,
    packed_ref,
    halo_ref,
    x_sem,
    local_sem,
    send_sem,
    recv_sem,
    halo_send_sem,
    halo_recv_sem,
    ready_sem,
    start_sem,
    group_sem,
    halo_sem,
):
    points, rows, nodes = x_ref.shape
    blocks = nodes // LANES
    chunks = len(bounds) - 1
    loads = bounds[:3] + bounds[-1:]
    groups = bounds[:1] + bounds[3:]
    count, slots = coupling_ref.shape[1], list_ref.shape[1]
    shares, devices = lax.axis_size("harm"), lax.axis_size("node")
    me, place = lax.axis_index("harm"), lax.axis_index("node")
    length = rows * shares

    def on_mesh(device):
        return jnp.logical_and(device >= 0, device < devices)

    def load(step):
        span = slice(loads[step] * LANES, loads[step + 1] * LANES)
        return pltpu.make_async_copy(
            x_hbm.at[:, :, span], x_ref.at[:, :, span], x_sem.at[step]
        )

    def exchange(low, high, by, recv):
        return pltpu.make_async_remote_copy(
            src_ref=pool_ref.at[low:high],
            dst_ref=arrived_ref.at[by - 1, low:high],
            send_sem=send_sem.at[by - 1],
            recv_sem=recv_sem.at[by - 1, recv],
            device_id={"harm": lax.rem(me + by, shares)},
            device_id_type=MESH,
        )

    def group_of(block):
        return sum(block >= end for end in groups[1:])

    def arrival(group, by):
        return exchange(groups[group], groups[group + 1], by, group)

    def halo(direction, device):
        return pltpu.make_async_remote_copy(
            src_ref=packed_ref.at[direction],
            dst_ref=halo_ref.at[direction],
            send_sem=halo_send_sem.at[direction],
            recv_sem=halo_recv_sem.at[direction],
            device_id={"node": device},
            device_id_type=MESH,
        )

    root = me == 0
    member = jnp.logical_not(root)
    members = [{"harm": other} for other in range(1, shares)]
    barrier = pltpu.get_barrier_semaphore()
    load(0).start()

    def signal(semaphore, device):
        pl.semaphore_signal(semaphore, inc=1, device_id=device, device_id_type=MESH)

    @pl.when(root)
    def _():
        for other in members:
            signal(barrier, other)

    def greet(semaphore):
        for offset in OFFSETS:

            @pl.when(jnp.logical_and(root, on_mesh(place + offset)))
            def _():
                signal(semaphore, {"node": place + offset})

    greet(barrier)
    greeted = sum(on_mesh(place + offset).astype(jnp.int32) for offset in OFFSETS)
    for step in range(1, len(loads) - 1):
        load(step).start()
    tables = [
        pltpu.make_async_copy(source, target, local_sem.at[i])
        for i, (source, target) in enumerate([(list_hbm, list_ref), (slot_hbm, slot_ref)])
    ]
    large = [
        pltpu.make_async_copy(source, target, local_sem.at[i + 2])
        for i, (source, target) in enumerate(
            [
                (source_hbm, out_ref),
                (coupling_hbm, coupling_ref),
                (synthesis_hbm.at[me], synthesis_ref),
                (analysis_hbm.at[me], analysis_ref),
            ]
        )
    ]
    scales = [
        pltpu.make_async_copy(source, scale_ref.at[i], local_sem.at[6])
        for i, source in enumerate([capacitance_hbm, saturation_hbm, steepness_hbm, junction_hbm])
    ]
    for copy in tables:
        copy.start()

    def round_block(block, carry):
        span = pl.ds(pl.multiple_of(block * LANES, LANES), LANES)
        for point in range(points):
            pool_ref[block, point * rows : (point + 1) * rows, :] = x_ref[point, :, span].astype(
                jnp.bfloat16
            )
        return carry

    def round_chunk(chunk):
        if chunk < len(loads) - 1:
            load(chunk).wait()
        lax.fori_loop(bounds[chunk], bounds[chunk + 1], round_block, 0, unroll=unit)

    def send(low, high):
        for by in range(1, shares):
            exchange(low, high, by, group_of(low)).start()

    @pl.when(member)
    def _():
        pl.semaphore_wait(barrier, 1)
        signal(ready_sem, {"harm": 0})

    round_chunk(0)
    for copy in large + scales:
        copy.start()

    @pl.when(root)
    def _():
        pl.semaphore_wait(barrier, greeted)
        pl.semaphore_wait(ready_sem, shares - 1)
        if shares > 2:
            for other in members:
                signal(start_sem, other)

    if shares > 2:

        @pl.when(member)
        def _():
            pl.semaphore_wait(start_sem, 1)

    for chunk in range(1, chunks):
        round_chunk(chunk)
        send(bounds[chunk - 1], bounds[chunk])
    for copy in tables:
        copy.wait()
    for direction in range(len(OFFSETS)):
        for slot in range(slots):
            packed_ref[direction, slot] = pool_ref[list_ref[direction, slot, place]]
    late = lax.rem(place, 2) == 1
    final, kept = bounds[-2], blocks - 1

    @pl.when(jnp.logical_not(late))
    def _():
        send(final, blocks)

    if final < kept:

        @pl.when(late)
        def _():
            send(final, kept)

    greet(group_sem)

    @pl.when(root)
    def _():
        pl.semaphore_wait(group_sem, greeted)
        for other in members:
            signal(halo_sem, other)

    @pl.when(member)
    def _():
        pl.semaphore_wait(halo_sem, 1)

    for direction, offset in enumerate(OFFSETS):

        @pl.when(on_mesh(place + offset))
        def _():
            halo(direction, place + offset).start()

    pool_ref[blocks + len(OFFSETS) * slots] = jnp.zeros(pool_ref.shape[1:], pool_ref.dtype)
    for copy in large:
        copy.wait()
    pltpu.make_async_copy(scale_ref, scale_ref, local_sem.at[6]).wait()
    for direction, offset in enumerate(OFFSETS):
        first = blocks + direction * slots
        there = on_mesh(place - offset)

        @pl.when(there)
        def _():
            halo(direction, place - offset).wait_recv()
            for slot in range(slots):
                pool_ref[first + slot] = halo_ref[direction, slot]

        @pl.when(jnp.logical_not(there))
        def _():
            for slot in range(slots):
                pool_ref[first + slot] = jnp.zeros(pool_ref.shape[1:], pool_ref.dtype)

    row = me * rows + lax.broadcasted_iota(jnp.int32, (rows, LANES), 0)
    even = row % 2 == 0
    rate = (row // 2).astype(jnp.float32) * (2.0 / length)
    rate = jnp.where(even, rate, -rate)

    def couple(block, carry):
        gathered = jnp.concatenate([pool_ref[slot_ref[k, block]] for k in range(count)], axis=1)
        matrix = jnp.concatenate([coupling_ref[block, k] for k in range(count)], axis=1)
        coupled = lax.dot_general(
            gathered, matrix, (((1,), (1,)), ((), ())), preferred_element_type=jnp.float32
        )
        scaled = rate * scale_ref[0, pl.ds(block, 1), :]
        span = pl.ds(pl.multiple_of(block * LANES, LANES), LANES)
        for point in range(points):
            values = x_ref[point, :, span]
            other = jnp.where(even, pltpu.roll(values, rows - 1, 0), pltpu.roll(values, 1, 0))
            out_ref[point, :, span] = (
                coupled[point * rows : (point + 1) * rows]
                + scaled * other
                - out_ref[point, :, span]
            )
        return carry

    lax.fori_loop(0, blocks, couple, 0, unroll=unit)

    def nonlinear(group, carry):
        ids = [group * unit + inner for inner in range(unit)]
        factors = [widen(scale_ref, index, ids) for index in (1, 2, 3)]
        span = pl.ds(pl.multiple_of(group * unit * LANES, unit * LANES), unit * LANES)
        for point in range(points):
            held = slice(point * rows, (point + 1) * rows)
            spectra = [jnp.concatenate([pool_ref[block, held, :] for block in ids], axis=1)]
            for by in range(1, shares):
                spectra.append(
                    jnp.concatenate([arrived_ref[by - 1, block, held, :] for block in ids], axis=1)
                )
            out_ref[point, :, span] += evaluate(
                spectra, synthesis_ref[...], analysis_ref[...], *factors
            )
        return carry

    for group in range(len(groups) - 2):
        for by in range(1, shares):
            arrival(group, by).wait_recv()
        if group == len(groups) - 3:

            @pl.when(late)
            def _():
                send(kept, blocks)

        lax.fori_loop(groups[group] // unit, groups[group + 1] // unit, nonlinear, 0)
    tail_ref[0] = pool_ref[final:blocks]
    for by in range(1, shares):
        arrival(len(groups) - 2, by).wait_recv()
        tail_ref[by] = arrived_ref[by - 1, final:blocks]

    for by in range(1, shares):
        exchange(0, blocks, by, 0).wait_send()
    for direction, offset in enumerate(OFFSETS):

        @pl.when(on_mesh(place + offset))
        def _():
            halo(direction, place + offset).wait_send()


def local_part(
    spectrum,
    source,
    coupling,
    capacitance,
    saturation,
    steepness,
    junction,
    halo_list,
    neighbour_slot,
):
    rows, points, nodes = spectrum.shape
    shares = lax.axis_size("harm")
    length = rows * shares
    blocks = nodes // LANES
    unit = 2 if blocks % 2 == 0 else 1
    bounds = sorted({cut * blocks // CUTS[-1] // unit * unit for cut in CUTS})
    last = blocks - bounds[-2]
    slots, count = halo_list.shape[2], neighbour_slot.shape[1]
    directions = len(OFFSETS)
    height = points * rows
    x = jnp.transpose(spectrum, (1, 0, 2))
    injected = jnp.transpose(source, (1, 0, 2))
    synthesis, analysis = (jnp.asarray(t) for t in fourier_tables(length, shares))
    scales = [v.reshape(blocks, LANES) for v in (capacitance, saturation, steepness, junction)]
    vmem = pl.BlockSpec(memory_space=pltpu.VMEM)
    hbm = pl.BlockSpec(memory_space=pltpu.HBM)
    bf16, f32 = jnp.bfloat16, jnp.float32
    held = pl.pallas_call(
        functools.partial(kernel, unit, bounds),
        in_specs=[hbm] * 11,
        out_specs=[vmem] * 5,
        out_shape=[
            pltpu.VMEM((points, rows, nodes), f32),
            pltpu.VMEM((shares, last, height, LANES), bf16),
            pltpu.VMEM((length, 2 * length), bf16),
            pltpu.VMEM((rows, 2 * length), bf16),
            pltpu.VMEM((4, blocks, LANES), f32),
        ],
        scratch_shapes=[
            pltpu.SMEM((directions, slots, halo_list.shape[0]), jnp.int32),
            pltpu.SMEM((count, blocks), jnp.int32),
            pltpu.VMEM((points, rows, nodes), f32),
            pltpu.VMEM((blocks, count, LANES, LANES), bf16),
            pltpu.VMEM((blocks + directions * slots + 1, height, LANES), bf16),
            pltpu.VMEM((shares - 1, blocks, height, LANES), bf16),
            pltpu.VMEM((directions, slots, height, LANES), bf16),
            pltpu.VMEM((directions, slots, height, LANES), bf16),
            pltpu.SemaphoreType.DMA((3,)),
            pltpu.SemaphoreType.DMA((7,)),
            pltpu.SemaphoreType.DMA((shares - 1,)),
            pltpu.SemaphoreType.DMA((shares - 1, len(bounds) - 3)),
            pltpu.SemaphoreType.DMA((directions,)),
            pltpu.SemaphoreType.DMA((directions,)),
        ]
        + [pltpu.SemaphoreType.REGULAR] * 4,
        compiler_params=pltpu.CompilerParams(
            collective_id=0, has_side_effects=True, vmem_limit_bytes=VMEM_BYTES
        ),
        cost_estimate=pl.CostEstimate(
            flops=2 * height * nodes * (count * LANES + 3 * length),
            bytes_accessed=coupling.size * 2 + 3 * x.size * 4,
            transcendentals=0,
        ),
        name="residual",
    )(
        *[
            pltpu.with_memory_space_constraint(value, pltpu.HBM)
            for value in (
                jnp.transpose(halo_list, (1, 2, 0)),
                neighbour_slot.T,
                x,
                injected,
                coupling,
                synthesis,
                analysis,
                *scales,
            )
        ]
    )
    total = pl.pallas_call(
        finish_kernel,
        in_specs=[vmem] * 5,
        out_specs=hbm,
        out_shape=pltpu.HBM((points, rows, nodes), f32),
        scratch_shapes=[
            pltpu.VMEM((points, rows, last * LANES), f32),
            pltpu.SemaphoreType.DMA((2,)),
        ],
        compiler_params=pltpu.CompilerParams(vmem_limit_bytes=8 << 20),
        cost_estimate=pl.CostEstimate(
            flops=6 * height * last * LANES * length, bytes_accessed=x.size * 4, transcendentals=0
        ),
        name="finish",
    )(*[pltpu.with_memory_space_constraint(value, pltpu.VMEM) for value in held])
    return jnp.transpose(total, (1, 0, 2))


def solution(mesh):
    in_specs = (
        P("harm", None, "node"),
        P("harm", None, "node"),
        P("node", None, None, None),
        P("node"),
        P("node"),
        P("node"),
        P("node"),
        P(),
        P("node", None),
    )
    return jax.shard_map(
        local_part, mesh=mesh, in_specs=in_specs, out_specs=P("harm", None, "node"), check_vma=False
    )
```

```python
import functools

import jax
import jax.numpy as jnp
import numpy as np
from jax import lax
from jax.experimental import pallas as pl
from jax.experimental.pallas import tpu as pltpu
from jax.sharding import PartitionSpec as P

LOG_TWO = 0.6931471805599453
OFFSETS = (-2, -1, 1, 2)
CUTS = (0, 2, 4, 14, 26, 36)
LATER = (36, 42, 46, 48)
TOTAL = 48
LANES = 128
VMEM_BYTES = 36 << 20
MESH = pl.DeviceIdType.MESH


def fourier_tables(length, shares):
    rows = length // shares
    sample = np.arange(length)[:, None]
    column = np.arange(length)[None, :]
    angle = 2.0 * np.pi / length * (column // 2 * sample % length)
    table = np.where(column % 2 == 1, np.sin(angle), np.cos(angle))
    table = np.where(column == 1, np.where(sample % 2 == 0, 1.0, -1.0), table)
    weights = np.where(np.arange(length) < 2, 1.0, 2.0) / length
    analysis = table.T * weights[:, None]
    pulsation = np.arange(length // 2)[:, None, None] / (length // 2)
    pairs = analysis.reshape(length // 2, 2, length)
    slope = np.concatenate([pulsation * pairs[:, 1:], -pulsation * pairs[:, :1]], axis=1)
    both = np.concatenate([analysis, slope.reshape(length, length)], axis=1)
    table = table.astype(np.float32)
    high = table.astype(jnp.bfloat16)
    low = (table - high.astype(np.float32)).astype(jnp.bfloat16)
    order = [
        np.concatenate([np.arange(rows) + (me - by) % shares * rows for by in range(shares)])
        for me in range(shares)
    ]
    synthesis = np.stack([np.concatenate([high[:, o], low[:, o]], axis=1) for o in order])
    return synthesis, both.astype(jnp.bfloat16).reshape(shares, rows, 2 * length)


def evaluate(spectra, synthesis, analysis, saturation, steepness, junction):
    stacked = jnp.concatenate(spectra + spectra, axis=0)
    voltage = jnp.dot(synthesis, stacked, preferred_element_type=jnp.float32)
    drive = steepness * voltage
    softplus = jnp.maximum(drive, 0.0) + jnp.log(1.0 + jnp.exp(-jnp.abs(drive)))
    current = (saturation * (softplus - LOG_TWO)).astype(jnp.bfloat16)
    charge = (junction * voltage * lax.rsqrt(1.0 + voltage * voltage)).astype(jnp.bfloat16)
    samples = jnp.concatenate([current, charge], axis=0)
    return jnp.dot(analysis, samples, preferred_element_type=jnp.float32)


def widen(scale_ref, index, blocks):
    parts = [scale_ref[index, pl.ds(block, 1), :] for block in blocks]
    return jnp.concatenate(parts, axis=1)


def early_kernel(width, total_ref, out_hbm, token_ref, sem):
    copy = pltpu.make_async_copy(
        total_ref.at[:, :, :width], out_hbm.at[:, :, :width], sem.at[0]
    )
    copy.start()
    token_ref[...] = jnp.zeros_like(token_ref)
    copy.wait()


def finish_kernel(
    _, rest_ref, tail_ref, synthesis_ref, analysis_ref, scale_ref, out_hbm, last_ref, sem
):
    points, rows, width = rest_ref.shape
    shares, unit = tail_ref.shape[:2]
    nodes = out_hbm.shape[2]
    blocks = nodes // LANES
    done, before = width - unit * LANES, nodes - width
    bulk = pltpu.make_async_copy(
        rest_ref.at[:, :, :done], out_hbm.at[:, :, before : before + done], sem.at[0]
    )
    bulk.start()
    ids = range(blocks - unit, blocks)
    scales = [widen(scale_ref, index, ids) for index in (1, 2, 3)]
    for point in range(points):
        held = slice(point * rows, (point + 1) * rows)
        spectra = [
            jnp.concatenate([tail_ref[share, inner, held, :] for inner in range(unit)], axis=1)
            for share in range(shares)
        ]
        last_ref[point] = rest_ref[point, :, done:] + evaluate(
            spectra, synthesis_ref[...], analysis_ref[...], *scales
        )
    copy = pltpu.make_async_copy(last_ref, out_hbm.at[:, :, before + done :], sem.at[1])
    copy.start()
    bulk.wait()
    copy.wait()


def later_kernel(
    unit,
    written,
    bounds,
    _,
    total_ref,
    pool_ref,
    before_ref,
    synthesis_ref,
    analysis_ref,
    scale_ref,
    rest_ref,
    tail_ref,
    arrived_ref,
    send_sem,
    recv_sem,
):
    points, rows, nodes = total_ref.shape
    blocks = nodes // LANES
    shares = lax.axis_size("harm")
    me = lax.axis_index("harm")
    base = bounds[0]
    barrier = pltpu.get_barrier_semaphore()
    for by in range(1, shares):
        pl.semaphore_signal(
            barrier, inc=1, device_id={"harm": lax.rem(me + by, shares)}, device_id_type=MESH
        )
    pl.semaphore_wait(barrier, shares - 1)

    def exchange(low, high, by, recv):
        return pltpu.make_async_remote_copy(
            src_ref=pool_ref.at[low:high],
            dst_ref=arrived_ref.at[by - 1, low - base : high - base],
            send_sem=send_sem.at[by - 1],
            recv_sem=recv_sem.at[by - 1, recv],
            device_id={"harm": lax.rem(me + by, shares)},
            device_id_type=MESH,
        )

    pieces = list(zip(bounds[:-1], bounds[1:]))
    for index, (low, high) in enumerate(pieces):
        for by in range(1, shares):
            exchange(low, high, by, index).start()

    def nonlinear(source_ref, shift, group, carry):
        ids = [group * unit + inner for inner in range(unit)]
        factors = [widen(scale_ref, index, ids) for index in (1, 2, 3)]
        width = unit * LANES
        span = pl.ds(pl.multiple_of(group * width, width), width)
        target = pl.ds(pl.multiple_of(group * width - written * LANES, width), width)
        for point in range(points):
            held = slice(point * rows, (point + 1) * rows)
            spectra = [jnp.concatenate([pool_ref[block, held, :] for block in ids], axis=1)]
            for by in range(1, shares):
                spectra.append(
                    jnp.concatenate(
                        [source_ref[by - 1, block - shift, held, :] for block in ids], axis=1
                    )
                )
            rest_ref[point, :, target] = total_ref[point, :, span] + evaluate(
                spectra, synthesis_ref[...], analysis_ref[...], *factors
            )
        return carry

    lax.fori_loop(
        written // unit, base // unit, functools.partial(nonlinear, before_ref, 0), 0
    )
    final = bounds[-2]
    rest_ref[:, :, (final - written) * LANES :] = total_ref[:, :, final * LANES :]
    tail_ref[0] = pool_ref[final:blocks]
    for index, (low, high) in enumerate(pieces):
        for by in range(1, shares):
            exchange(low, high, by, index).wait_recv()
        if high < blocks:
            lax.fori_loop(
                low // unit, high // unit, functools.partial(nonlinear, arrived_ref, base), 0
            )
    for by in range(1, shares):
        tail_ref[by] = arrived_ref[by - 1, final - base :]
    for by in range(1, shares):
        exchange(base, blocks, by, 0).wait_send()


def kernel(
    unit,
    bounds,
    list_hbm,
    slot_hbm,
    x_hbm,
    source_hbm,
    coupling_hbm,
    synthesis_hbm,
    analysis_hbm,
    capacitance_hbm,
    saturation_hbm,
    steepness_hbm,
    junction_hbm,
    out_ref,
    pool_ref,
    arrived_ref,
    synthesis_ref,
    analysis_ref,
    scale_ref,
    list_ref,
    slot_ref,
    x_ref,
    coupling_ref,
    packed_ref,
    halo_ref,
    x_sem,
    local_sem,
    send_sem,
    recv_sem,
    halo_send_sem,
    halo_recv_sem,
    ready_sem,
    start_sem,
    group_sem,
    halo_sem,
):
    points, rows, nodes = x_ref.shape
    blocks = nodes // LANES
    chunks = len(bounds) - 1
    loads = bounds[:3] + [blocks]
    groups = bounds[:1] + bounds[3:]
    count, slots = coupling_ref.shape[1], list_ref.shape[1]
    shares, devices = lax.axis_size("harm"), lax.axis_size("node")
    me, place = lax.axis_index("harm"), lax.axis_index("node")
    length = rows * shares

    def on_mesh(device):
        return jnp.logical_and(device >= 0, device < devices)

    def load(step):
        span = slice(loads[step] * LANES, loads[step + 1] * LANES)
        return pltpu.make_async_copy(
            x_hbm.at[:, :, span], x_ref.at[:, :, span], x_sem.at[step]
        )

    def exchange(low, high, by, recv):
        return pltpu.make_async_remote_copy(
            src_ref=pool_ref.at[low:high],
            dst_ref=arrived_ref.at[by - 1, low:high],
            send_sem=send_sem.at[by - 1],
            recv_sem=recv_sem.at[by - 1, recv],
            device_id={"harm": lax.rem(me + by, shares)},
            device_id_type=MESH,
        )

    def group_of(block):
        return sum(block >= end for end in groups[1:])

    def arrival(group, by):
        return exchange(groups[group], groups[group + 1], by, group)

    def halo(direction, device):
        return pltpu.make_async_remote_copy(
            src_ref=packed_ref.at[direction],
            dst_ref=halo_ref.at[direction],
            send_sem=halo_send_sem.at[direction],
            recv_sem=halo_recv_sem.at[direction],
            device_id={"node": device},
            device_id_type=MESH,
        )

    root = me == 0
    member = jnp.logical_not(root)
    members = [{"harm": other} for other in range(1, shares)]
    barrier = pltpu.get_barrier_semaphore()
    load(0).start()

    def signal(semaphore, device):
        pl.semaphore_signal(semaphore, inc=1, device_id=device, device_id_type=MESH)

    @pl.when(root)
    def _():
        for other in members:
            signal(barrier, other)

    def greet(semaphore):
        for offset in OFFSETS:

            @pl.when(jnp.logical_and(root, on_mesh(place + offset)))
            def _():
                signal(semaphore, {"node": place + offset})

    greet(barrier)
    greeted = sum(on_mesh(place + offset).astype(jnp.int32) for offset in OFFSETS)
    for step in range(1, len(loads) - 1):
        load(step).start()
    tables = [
        pltpu.make_async_copy(source, target, local_sem.at[i])
        for i, (source, target) in enumerate([(list_hbm, list_ref), (slot_hbm, slot_ref)])
    ]
    large = [
        pltpu.make_async_copy(source, target, local_sem.at[i + 2])
        for i, (source, target) in enumerate(
            [
                (source_hbm, out_ref),
                (coupling_hbm, coupling_ref),
                (synthesis_hbm.at[me], synthesis_ref),
                (analysis_hbm.at[me], analysis_ref),
            ]
        )
    ]
    scales = [
        pltpu.make_async_copy(source, scale_ref.at[i], local_sem.at[6])
        for i, source in enumerate([capacitance_hbm, saturation_hbm, steepness_hbm, junction_hbm])
    ]
    for copy in tables:
        copy.start()

    def round_block(block, carry):
        span = pl.ds(pl.multiple_of(block * LANES, LANES), LANES)
        for point in range(points):
            pool_ref[block, point * rows : (point + 1) * rows, :] = x_ref[point, :, span].astype(
                jnp.bfloat16
            )
        return carry

    def round_chunk(chunk):
        if chunk < len(loads) - 1:
            load(chunk).wait()
        lax.fori_loop(bounds[chunk], bounds[chunk + 1], round_block, 0, unroll=unit)

    def send(low, high):
        for by in range(1, shares):
            exchange(low, high, by, group_of(low)).start()

    @pl.when(member)
    def _():
        pl.semaphore_wait(barrier, 1)
        signal(ready_sem, {"harm": 0})

    def start_large():
        for copy in large + scales:
            copy.start()

    round_chunk(0)
    round_chunk(1)

    @pl.when(root)
    def _():
        start_large()
        pl.semaphore_wait(barrier, greeted)
        pl.semaphore_wait(ready_sem, shares - 1)
        if shares > 2:
            for other in members:
                signal(start_sem, other)

    if shares > 2:

        @pl.when(member)
        def _():
            pl.semaphore_wait(start_sem, 1)

    send(bounds[0], bounds[1])
    pl.when(member)(start_large)
    send(bounds[1], bounds[2])
    for chunk in range(2, chunks):
        round_chunk(chunk)
        if chunk > 2:
            send(bounds[chunk - 1], bounds[chunk])
    lax.fori_loop(bounds[-1], blocks, round_block, 0, unroll=unit)
    for copy in tables:
        copy.wait()
    for direction in range(len(OFFSETS)):
        for slot in range(slots):
            packed_ref[direction, slot] = pool_ref[list_ref[direction, slot, place]]
    late = lax.rem(place, 2) == 1
    kept = bounds[-2]

    @pl.when(jnp.logical_not(late))
    def _():
        send(kept, bounds[-1])

    greet(group_sem)

    @pl.when(root)
    def _():
        pl.semaphore_wait(group_sem, greeted)
        for other in members:
            signal(halo_sem, other)

    @pl.when(member)
    def _():
        pl.semaphore_wait(halo_sem, 1)

    for direction, offset in enumerate(OFFSETS):

        @pl.when(on_mesh(place + offset))
        def _():
            halo(direction, place + offset).start()

    pool_ref[blocks + len(OFFSETS) * slots] = jnp.zeros(pool_ref.shape[1:], pool_ref.dtype)
    for copy in large:
        copy.wait()
    pltpu.make_async_copy(scale_ref, scale_ref, local_sem.at[6]).wait()
    for direction, offset in enumerate(OFFSETS):
        first = blocks + direction * slots
        there = on_mesh(place - offset)

        @pl.when(there)
        def _():
            halo(direction, place - offset).wait_recv()
            for slot in range(slots):
                pool_ref[first + slot] = halo_ref[direction, slot]

        @pl.when(jnp.logical_not(there))
        def _():
            for slot in range(slots):
                pool_ref[first + slot] = jnp.zeros(pool_ref.shape[1:], pool_ref.dtype)

    row = me * rows + lax.broadcasted_iota(jnp.int32, (rows, LANES), 0)
    even = row % 2 == 0
    rate = (row // 2).astype(jnp.float32) * (2.0 / length)
    rate = jnp.where(even, rate, -rate)

    def couple(block, carry):
        gathered = jnp.concatenate([pool_ref[slot_ref[k, block]] for k in range(count)], axis=1)
        matrix = jnp.concatenate([coupling_ref[block, k] for k in range(count)], axis=1)
        coupled = lax.dot_general(
            gathered, matrix, (((1,), (1,)), ((), ())), preferred_element_type=jnp.float32
        )
        scaled = rate * scale_ref[0, pl.ds(block, 1), :]
        span = pl.ds(pl.multiple_of(block * LANES, LANES), LANES)
        for point in range(points):
            values = x_ref[point, :, span]
            other = jnp.where(even, pltpu.roll(values, rows - 1, 0), pltpu.roll(values, 1, 0))
            out_ref[point, :, span] = (
                coupled[point * rows : (point + 1) * rows]
                + scaled * other
                - out_ref[point, :, span]
            )
        return carry

    lax.fori_loop(0, blocks, couple, 0, unroll=unit)

    def nonlinear(group, carry):
        ids = [group * unit + inner for inner in range(unit)]
        factors = [widen(scale_ref, index, ids) for index in (1, 2, 3)]
        span = pl.ds(pl.multiple_of(group * unit * LANES, unit * LANES), unit * LANES)
        for point in range(points):
            held = slice(point * rows, (point + 1) * rows)
            spectra = [jnp.concatenate([pool_ref[block, held, :] for block in ids], axis=1)]
            for by in range(1, shares):
                spectra.append(
                    jnp.concatenate([arrived_ref[by - 1, block, held, :] for block in ids], axis=1)
                )
            out_ref[point, :, span] += evaluate(
                spectra, synthesis_ref[...], analysis_ref[...], *factors
            )
        return carry

    last = len(groups) - 2
    for group in range(last):
        for by in range(1, shares):
            arrival(group, by).wait_recv()
        lax.fori_loop(groups[group] // unit, groups[group + 1] // unit, nonlinear, 0)

    @pl.when(late)
    def _():
        send(kept, bounds[-1])

    for by in range(1, shares):
        arrival(last, by).wait_recv()
    for by in range(1, shares):
        exchange(0, bounds[-1], by, 0).wait_send()
    for direction, offset in enumerate(OFFSETS):

        @pl.when(on_mesh(place + offset))
        def _():
            halo(direction, place + offset).wait_send()


def local_part(
    spectrum,
    source,
    coupling,
    capacitance,
    saturation,
    steepness,
    junction,
    halo_list,
    neighbour_slot,
):
    rows, points, nodes = spectrum.shape
    shares = lax.axis_size("harm")
    length = rows * shares
    blocks = nodes // LANES
    unit = 2 if blocks % 2 == 0 else 1
    bounds, later = (
        sorted({cut * blocks // TOTAL // unit * unit for cut in cuts}) for cuts in (CUTS, LATER)
    )
    later[-1] = blocks
    last, written = blocks - later[-2], bounds[-2]
    slots, count = halo_list.shape[2], neighbour_slot.shape[1]
    directions = len(OFFSETS)
    height = points * rows
    x = jnp.transpose(spectrum, (1, 0, 2))
    injected = jnp.transpose(source, (1, 0, 2))
    synthesis, analysis = (jnp.asarray(t) for t in fourier_tables(length, shares))
    scales = [v.reshape(blocks, LANES) for v in (capacitance, saturation, steepness, junction)]
    vmem = pl.BlockSpec(memory_space=pltpu.VMEM)
    hbm = pl.BlockSpec(memory_space=pltpu.HBM)
    bf16, f32 = jnp.bfloat16, jnp.float32
    held = pl.pallas_call(
        functools.partial(kernel, unit, bounds),
        in_specs=[hbm] * 11,
        out_specs=[vmem] * 6,
        out_shape=[
            pltpu.VMEM((points, rows, nodes), f32),
            pltpu.VMEM((blocks + directions * slots + 1, height, LANES), bf16),
            pltpu.VMEM((shares - 1, blocks, height, LANES), bf16),
            pltpu.VMEM((length, 2 * length), bf16),
            pltpu.VMEM((rows, 2 * length), bf16),
            pltpu.VMEM((4, blocks, LANES), f32),
        ],
        scratch_shapes=[
            pltpu.SMEM((directions, slots, halo_list.shape[0]), jnp.int32),
            pltpu.SMEM((count, blocks), jnp.int32),
            pltpu.VMEM((points, rows, nodes), f32),
            pltpu.VMEM((blocks, count, LANES, LANES), bf16),
            pltpu.VMEM((directions, slots, height, LANES), bf16),
            pltpu.VMEM((directions, slots, height, LANES), bf16),
            pltpu.SemaphoreType.DMA((3,)),
            pltpu.SemaphoreType.DMA((7,)),
            pltpu.SemaphoreType.DMA((shares - 1,)),
            pltpu.SemaphoreType.DMA((shares - 1, len(bounds) - 3)),
            pltpu.SemaphoreType.DMA((directions,)),
            pltpu.SemaphoreType.DMA((directions,)),
        ]
        + [pltpu.SemaphoreType.REGULAR] * 4,
        compiler_params=pltpu.CompilerParams(
            collective_id=0, has_side_effects=True, vmem_limit_bytes=VMEM_BYTES
        ),
        cost_estimate=pl.CostEstimate(
            flops=2 * height * nodes * (count * LANES + 3 * length),
            bytes_accessed=coupling.size * 2 + 3 * x.size * 4,
            transcendentals=0,
        ),
        name="residual",
    )(
        *[
            pltpu.with_memory_space_constraint(value, pltpu.HBM)
            for value in (
                jnp.transpose(halo_list, (1, 2, 0)),
                neighbour_slot.T,
                x,
                injected,
                coupling,
                synthesis,
                analysis,
                *scales,
            )
        ]
    )
    total, pool, arrived, *tables = (
        pltpu.with_memory_space_constraint(value, pltpu.VMEM) for value in held
    )
    early, token = pl.pallas_call(
        functools.partial(early_kernel, written * LANES),
        in_specs=[vmem],
        out_specs=[hbm, vmem],
        out_shape=[pltpu.HBM((points, rows, nodes), f32), pltpu.VMEM((8, LANES), f32)],
        scratch_shapes=[pltpu.SemaphoreType.DMA((1,))],
        compiler_params=pltpu.CompilerParams(vmem_limit_bytes=1 << 20),
        cost_estimate=pl.CostEstimate(
            flops=0, bytes_accessed=height * written * LANES * 4, transcendentals=0
        ),
        name="early",
    )(total)
    width = nodes - written * LANES
    rest, tail = pl.pallas_call(
        functools.partial(later_kernel, unit, written, later),
        in_specs=[vmem] * 7,
        out_specs=[vmem] * 2,
        out_shape=[
            pltpu.VMEM((points, rows, width), f32),
            pltpu.VMEM((shares, last, height, LANES), bf16),
        ],
        scratch_shapes=[
            pltpu.VMEM((shares - 1, blocks - later[0], height, LANES), bf16),
            pltpu.SemaphoreType.DMA((shares - 1,)),
            pltpu.SemaphoreType.DMA((shares - 1, len(later) - 1)),
        ],
        compiler_params=pltpu.CompilerParams(
            collective_id=1, has_side_effects=True, vmem_limit_bytes=12 << 20
        ),
        cost_estimate=pl.CostEstimate(
            flops=6 * height * width * length, bytes_accessed=0, transcendentals=0
        ),
        name="later",
    )(pltpu.with_memory_space_constraint(token, pltpu.VMEM), total, pool, arrived, *tables)
    total = pl.pallas_call(
        finish_kernel,
        in_specs=[hbm] + [vmem] * 5,
        out_specs=hbm,
        out_shape=pltpu.HBM((points, rows, nodes), f32),
        scratch_shapes=[
            pltpu.VMEM((points, rows, last * LANES), f32),
            pltpu.SemaphoreType.DMA((2,)),
        ],
        input_output_aliases={0: 0},
        compiler_params=pltpu.CompilerParams(vmem_limit_bytes=8 << 20),
        cost_estimate=pl.CostEstimate(
            flops=6 * height * last * LANES * length,
            bytes_accessed=height * width * 4,
            transcendentals=0,
        ),
        name="finish",
    )(
        early,
        *[pltpu.with_memory_space_constraint(value, pltpu.VMEM) for value in (rest, tail)],
        *tables,
    )
    return jnp.transpose(total, (1, 0, 2))


def solution(mesh):
    in_specs = (
        P("harm", None, "node"),
        P("harm", None, "node"),
        P("node", None, None, None),
        P("node"),
        P("node"),
        P("node"),
        P("node"),
        P(),
        P("node", None),
    )
    return jax.shard_map(
        local_part, mesh=mesh, in_specs=in_specs, out_specs=P("harm", None, "node"), check_vma=False
    )
```

```python
import functools

import jax
import jax.numpy as jnp
import numpy as np
from jax import lax
from jax.experimental import pallas as pl
from jax.experimental.pallas import tpu as pltpu
from jax.sharding import PartitionSpec as P

LOG_TWO = 0.6931471805599453
OFFSETS = (-2, -1, 1, 2)
CUTS = (0, 2, 4, 14, 26, 30)
LATER = (30, 38, 42, 46, 48)
TOTAL = 48
LANES = 128
VMEM_BYTES = 36 << 20
MESH = pl.DeviceIdType.MESH


def fourier_tables(length, shares):
    rows = length // shares
    sample = np.arange(length)[:, None]
    column = np.arange(length)[None, :]
    angle = 2.0 * np.pi / length * (column // 2 * sample % length)
    table = np.where(column % 2 == 1, np.sin(angle), np.cos(angle))
    table = np.where(column == 1, np.where(sample % 2 == 0, 1.0, -1.0), table)
    weights = np.where(np.arange(length) < 2, 1.0, 2.0) / length
    analysis = table.T * weights[:, None]
    pulsation = np.arange(length // 2)[:, None, None] / (length // 2)
    pairs = analysis.reshape(length // 2, 2, length)
    slope = np.concatenate([pulsation * pairs[:, 1:], -pulsation * pairs[:, :1]], axis=1)
    both = np.concatenate([analysis, slope.reshape(length, length)], axis=1)
    table = table.astype(np.float32)
    high = table.astype(jnp.bfloat16)
    low = (table - high.astype(np.float32)).astype(jnp.bfloat16)
    order = [
        np.concatenate([np.arange(rows) + (me - by) % shares * rows for by in range(shares)])
        for me in range(shares)
    ]
    synthesis = np.stack([np.concatenate([high[:, o], low[:, o]], axis=1) for o in order])
    return synthesis, both.astype(jnp.bfloat16).reshape(shares, rows, 2 * length)


def evaluate(spectra, synthesis, analysis, saturation, steepness, junction):
    stacked = jnp.concatenate(spectra + spectra, axis=0)
    voltage = jnp.dot(synthesis, stacked, preferred_element_type=jnp.float32)
    drive = steepness * voltage
    softplus = jnp.maximum(drive, 0.0) + jnp.log(1.0 + jnp.exp(-jnp.abs(drive)))
    current = (saturation * (softplus - LOG_TWO)).astype(jnp.bfloat16)
    charge = (junction * voltage * lax.rsqrt(1.0 + voltage * voltage)).astype(jnp.bfloat16)
    samples = jnp.concatenate([current, charge], axis=0)
    return jnp.dot(analysis, samples, preferred_element_type=jnp.float32)


def widen(scale_ref, index, blocks):
    parts = [scale_ref[index, pl.ds(block, 1), :] for block in blocks]
    return jnp.concatenate(parts, axis=1)


def early_kernel(width, total_ref, out_hbm, token_ref, sem):
    copy = pltpu.make_async_copy(
        total_ref.at[:, :, :width], out_hbm.at[:, :, :width], sem.at[0]
    )
    copy.start()
    token_ref[...] = jnp.zeros_like(token_ref)
    copy.wait()


def finish_kernel(
    _, rest_ref, tail_ref, synthesis_ref, analysis_ref, scale_ref, out_hbm, last_ref, sem
):
    points, rows, width = rest_ref.shape
    shares, unit = tail_ref.shape[:2]
    nodes = out_hbm.shape[2]
    blocks = nodes // LANES
    done, before = width - unit * LANES, nodes - width
    bulk = pltpu.make_async_copy(
        rest_ref.at[:, :, :done], out_hbm.at[:, :, before : before + done], sem.at[0]
    )
    bulk.start()
    ids = range(blocks - unit, blocks)
    scales = [widen(scale_ref, index, ids) for index in (1, 2, 3)]
    for point in range(points):
        held = slice(point * rows, (point + 1) * rows)
        spectra = [
            jnp.concatenate([tail_ref[share, inner, held, :] for inner in range(unit)], axis=1)
            for share in range(shares)
        ]
        last_ref[point] = rest_ref[point, :, done:] + evaluate(
            spectra, synthesis_ref[...], analysis_ref[...], *scales
        )
    copy = pltpu.make_async_copy(last_ref, out_hbm.at[:, :, before + done :], sem.at[1])
    copy.start()
    bulk.wait()
    copy.wait()


def later_kernel(
    unit,
    written,
    bounds,
    _,
    total_ref,
    pool_ref,
    before_ref,
    synthesis_ref,
    analysis_ref,
    scale_ref,
    rest_ref,
    tail_ref,
    arrived_ref,
    send_sem,
    recv_sem,
):
    points, rows, nodes = total_ref.shape
    blocks = nodes // LANES
    shares = lax.axis_size("harm")
    me = lax.axis_index("harm")
    base = bounds[0]
    late = lax.rem(lax.axis_index("node"), 2) == 1
    final = bounds[-2]

    def exchange(low, high, by, recv):
        return pltpu.make_async_remote_copy(
            src_ref=pool_ref.at[low:high],
            dst_ref=arrived_ref.at[by - 1, low - base : high - base],
            send_sem=send_sem.at[by - 1],
            recv_sem=recv_sem.at[by - 1, recv],
            device_id={"harm": lax.rem(me + by, shares)},
            device_id_type=MESH,
        )

    pieces = list(zip(bounds[:-1], bounds[1:]))

    def nonlinear(source_ref, shift, group, carry):
        ids = [group * unit + inner for inner in range(unit)]
        factors = [widen(scale_ref, index, ids) for index in (1, 2, 3)]
        width = unit * LANES
        span = pl.ds(pl.multiple_of(group * width, width), width)
        target = pl.ds(pl.multiple_of(group * width - written * LANES, width), width)
        for point in range(points):
            held = slice(point * rows, (point + 1) * rows)
            spectra = [jnp.concatenate([pool_ref[block, held, :] for block in ids], axis=1)]
            for by in range(1, shares):
                spectra.append(
                    jnp.concatenate(
                        [source_ref[by - 1, block - shift, held, :] for block in ids], axis=1
                    )
                )
            rest_ref[point, :, target] = total_ref[point, :, span] + evaluate(
                spectra, synthesis_ref[...], analysis_ref[...], *factors
            )
        return carry

    @pl.when(late)
    def _():
        barrier = pltpu.get_barrier_semaphore()
        for by in range(1, shares):
            pl.semaphore_signal(
                barrier, inc=1, device_id={"harm": lax.rem(me + by, shares)}, device_id_type=MESH
            )
        pl.semaphore_wait(barrier, shares - 1)
        for index, (low, high) in enumerate(pieces):
            for by in range(1, shares):
                exchange(low, high, by, index).start()
        lax.fori_loop(
            written // unit, base // unit, functools.partial(nonlinear, before_ref, 0), 0
        )
        rest_ref[:, :, (final - written) * LANES :] = total_ref[:, :, final * LANES :]
        tail_ref[0] = pool_ref[final:blocks]
        for index, (low, high) in enumerate(pieces):
            for by in range(1, shares):
                exchange(low, high, by, index).wait_recv()
            if high < blocks:
                lax.fori_loop(
                    low // unit, high // unit, functools.partial(nonlinear, arrived_ref, base), 0
                )
        for by in range(1, shares):
            tail_ref[by] = arrived_ref[by - 1, final - base :]
        for by in range(1, shares):
            exchange(base, blocks, by, 0).wait_send()

    @pl.when(jnp.logical_not(late))
    def _():
        rest_ref[...] = total_ref[:, :, written * LANES :]
        tail_ref[0] = pool_ref[final:blocks]
        for by in range(1, shares):
            tail_ref[by] = before_ref[by - 1, final:blocks]


def kernel(
    unit,
    bounds,
    later,
    list_hbm,
    slot_hbm,
    x_hbm,
    source_hbm,
    coupling_hbm,
    synthesis_hbm,
    analysis_hbm,
    capacitance_hbm,
    saturation_hbm,
    steepness_hbm,
    junction_hbm,
    out_ref,
    pool_ref,
    arrived_ref,
    synthesis_ref,
    analysis_ref,
    scale_ref,
    list_ref,
    slot_ref,
    x_ref,
    coupling_ref,
    packed_ref,
    halo_ref,
    x_sem,
    local_sem,
    send_sem,
    recv_sem,
    halo_send_sem,
    halo_recv_sem,
    ready_sem,
    start_sem,
    group_sem,
    halo_sem,
):
    points, rows, nodes = x_ref.shape
    blocks = nodes // LANES
    chunks = len(bounds) - 1
    loads = bounds[:3] + [blocks]
    groups = bounds[:1] + bounds[3:] + later[1:]
    count, slots = coupling_ref.shape[1], list_ref.shape[1]
    shares, devices = lax.axis_size("harm"), lax.axis_size("node")
    me, place = lax.axis_index("harm"), lax.axis_index("node")
    length = rows * shares

    def on_mesh(device):
        return jnp.logical_and(device >= 0, device < devices)

    def load(step):
        span = slice(loads[step] * LANES, loads[step + 1] * LANES)
        return pltpu.make_async_copy(
            x_hbm.at[:, :, span], x_ref.at[:, :, span], x_sem.at[step]
        )

    def exchange(low, high, by, recv):
        return pltpu.make_async_remote_copy(
            src_ref=pool_ref.at[low:high],
            dst_ref=arrived_ref.at[by - 1, low:high],
            send_sem=send_sem.at[by - 1],
            recv_sem=recv_sem.at[by - 1, recv],
            device_id={"harm": lax.rem(me + by, shares)},
            device_id_type=MESH,
        )

    def group_of(block):
        return sum(block >= end for end in groups[1:])

    def arrival(group, by):
        return exchange(groups[group], groups[group + 1], by, group)

    def halo(direction, device):
        return pltpu.make_async_remote_copy(
            src_ref=packed_ref.at[direction],
            dst_ref=halo_ref.at[direction],
            send_sem=halo_send_sem.at[direction],
            recv_sem=halo_recv_sem.at[direction],
            device_id={"node": device},
            device_id_type=MESH,
        )

    root = me == 0
    member = jnp.logical_not(root)
    members = [{"harm": other} for other in range(1, shares)]
    barrier = pltpu.get_barrier_semaphore()
    load(0).start()

    def signal(semaphore, device):
        pl.semaphore_signal(semaphore, inc=1, device_id=device, device_id_type=MESH)

    @pl.when(root)
    def _():
        for other in members:
            signal(barrier, other)

    def greet(semaphore):
        for offset in OFFSETS:

            @pl.when(jnp.logical_and(root, on_mesh(place + offset)))
            def _():
                signal(semaphore, {"node": place + offset})

    greet(barrier)
    greeted = sum(on_mesh(place + offset).astype(jnp.int32) for offset in OFFSETS)
    for step in range(1, len(loads) - 1):
        load(step).start()
    tables = [
        pltpu.make_async_copy(source, target, local_sem.at[i])
        for i, (source, target) in enumerate([(list_hbm, list_ref), (slot_hbm, slot_ref)])
    ]
    large = [
        pltpu.make_async_copy(source, target, local_sem.at[i + 2])
        for i, (source, target) in enumerate(
            [
                (source_hbm, out_ref),
                (coupling_hbm, coupling_ref),
                (synthesis_hbm.at[me], synthesis_ref),
                (analysis_hbm.at[me], analysis_ref),
            ]
        )
    ]
    scales = [
        pltpu.make_async_copy(source, scale_ref.at[i], local_sem.at[6])
        for i, source in enumerate([capacitance_hbm, saturation_hbm, steepness_hbm, junction_hbm])
    ]
    for copy in tables:
        copy.start()

    def round_block(block, carry):
        span = pl.ds(pl.multiple_of(block * LANES, LANES), LANES)
        for point in range(points):
            pool_ref[block, point * rows : (point + 1) * rows, :] = x_ref[point, :, span].astype(
                jnp.bfloat16
            )
        return carry

    def round_chunk(chunk):
        if chunk < len(loads) - 1:
            load(chunk).wait()
        lax.fori_loop(bounds[chunk], bounds[chunk + 1], round_block, 0, unroll=unit)

    def send(low, high):
        for by in range(1, shares):
            exchange(low, high, by, group_of(low)).start()

    @pl.when(member)
    def _():
        pl.semaphore_wait(barrier, 1)
        signal(ready_sem, {"harm": 0})

    def start_large():
        for copy in large + scales:
            copy.start()

    round_chunk(0)
    round_chunk(1)

    @pl.when(root)
    def _():
        start_large()
        pl.semaphore_wait(barrier, greeted)
        pl.semaphore_wait(ready_sem, shares - 1)
        if shares > 2:
            for other in members:
                signal(start_sem, other)

    if shares > 2:

        @pl.when(member)
        def _():
            pl.semaphore_wait(start_sem, 1)

    send(bounds[0], bounds[1])
    pl.when(member)(start_large)
    send(bounds[1], bounds[2])
    for chunk in range(2, chunks):
        round_chunk(chunk)
        if chunk > 2:
            send(bounds[chunk - 1], bounds[chunk])
    lax.fori_loop(bounds[-1], blocks, round_block, 0, unroll=unit)
    for copy in tables:
        copy.wait()
    for direction in range(len(OFFSETS)):
        for slot in range(slots):
            packed_ref[direction, slot] = pool_ref[list_ref[direction, slot, place]]
    late = lax.rem(place, 2) == 1
    soon = jnp.logical_not(late)
    send(bounds[-2], bounds[-1])

    @pl.when(soon)
    def _():
        for low, high in zip(later[:-1], later[1:]):
            send(low, high)

    greet(group_sem)

    @pl.when(root)
    def _():
        pl.semaphore_wait(group_sem, greeted)
        for other in members:
            signal(halo_sem, other)

    @pl.when(member)
    def _():
        pl.semaphore_wait(halo_sem, 1)

    for direction, offset in enumerate(OFFSETS):

        @pl.when(on_mesh(place + offset))
        def _():
            halo(direction, place + offset).start()

    pool_ref[blocks + len(OFFSETS) * slots] = jnp.zeros(pool_ref.shape[1:], pool_ref.dtype)
    for copy in large:
        copy.wait()
    pltpu.make_async_copy(scale_ref, scale_ref, local_sem.at[6]).wait()
    for direction, offset in enumerate(OFFSETS):
        first = blocks + direction * slots
        there = on_mesh(place - offset)

        @pl.when(there)
        def _():
            halo(direction, place - offset).wait_recv()
            for slot in range(slots):
                pool_ref[first + slot] = halo_ref[direction, slot]

        @pl.when(jnp.logical_not(there))
        def _():
            for slot in range(slots):
                pool_ref[first + slot] = jnp.zeros(pool_ref.shape[1:], pool_ref.dtype)

    row = me * rows + lax.broadcasted_iota(jnp.int32, (rows, LANES), 0)
    even = row % 2 == 0
    rate = (row // 2).astype(jnp.float32) * (2.0 / length)
    rate = jnp.where(even, rate, -rate)

    def couple(block, carry):
        gathered = jnp.concatenate([pool_ref[slot_ref[k, block]] for k in range(count)], axis=1)
        matrix = jnp.concatenate([coupling_ref[block, k] for k in range(count)], axis=1)
        coupled = lax.dot_general(
            gathered, matrix, (((1,), (1,)), ((), ())), preferred_element_type=jnp.float32
        )
        scaled = rate * scale_ref[0, pl.ds(block, 1), :]
        span = pl.ds(pl.multiple_of(block * LANES, LANES), LANES)
        for point in range(points):
            values = x_ref[point, :, span]
            other = jnp.where(even, pltpu.roll(values, rows - 1, 0), pltpu.roll(values, 1, 0))
            out_ref[point, :, span] = (
                coupled[point * rows : (point + 1) * rows]
                + scaled * other
                - out_ref[point, :, span]
            )
        return carry

    lax.fori_loop(0, blocks, couple, 0, unroll=unit)

    def nonlinear(group, carry):
        ids = [group * unit + inner for inner in range(unit)]
        factors = [widen(scale_ref, index, ids) for index in (1, 2, 3)]
        span = pl.ds(pl.multiple_of(group * unit * LANES, unit * LANES), unit * LANES)
        for point in range(points):
            held = slice(point * rows, (point + 1) * rows)
            spectra = [jnp.concatenate([pool_ref[block, held, :] for block in ids], axis=1)]
            for by in range(1, shares):
                spectra.append(
                    jnp.concatenate([arrived_ref[by - 1, block, held, :] for block in ids], axis=1)
                )
            out_ref[point, :, span] += evaluate(
                spectra, synthesis_ref[...], analysis_ref[...], *factors
            )
        return carry

    def receive(group):
        for by in range(1, shares):
            arrival(group, by).wait_recv()

    def process(group):
        lax.fori_loop(groups[group] // unit, groups[group + 1] // unit, nonlinear, 0)

    shared = groups.index(bounds[-1]) - 1
    for group in range(shared):
        receive(group)
        process(group)
    receive(shared)

    @pl.when(soon)
    def _():
        process(shared)
        for group in range(shared + 1, len(groups) - 1):
            receive(group)
            if group < len(groups) - 2:
                process(group)
        for by in range(1, shares):
            exchange(0, blocks, by, 0).wait_send()

    @pl.when(late)
    def _():
        for by in range(1, shares):
            exchange(0, bounds[-1], by, 0).wait_send()

    for direction, offset in enumerate(OFFSETS):

        @pl.when(on_mesh(place + offset))
        def _():
            halo(direction, place + offset).wait_send()


def local_part(
    spectrum,
    source,
    coupling,
    capacitance,
    saturation,
    steepness,
    junction,
    halo_list,
    neighbour_slot,
):
    rows, points, nodes = spectrum.shape
    shares = lax.axis_size("harm")
    length = rows * shares
    blocks = nodes // LANES
    unit = 2 if blocks % 2 == 0 else 1
    bounds, later = (
        sorted({cut * blocks // TOTAL // unit * unit for cut in cuts}) for cuts in (CUTS, LATER)
    )
    later[-1] = blocks
    last, written = blocks - later[-2], bounds[-2]
    slots, count = halo_list.shape[2], neighbour_slot.shape[1]
    directions = len(OFFSETS)
    height = points * rows
    x = jnp.transpose(spectrum, (1, 0, 2))
    injected = jnp.transpose(source, (1, 0, 2))
    synthesis, analysis = (jnp.asarray(t) for t in fourier_tables(length, shares))
    scales = [v.reshape(blocks, LANES) for v in (capacitance, saturation, steepness, junction)]
    vmem = pl.BlockSpec(memory_space=pltpu.VMEM)
    hbm = pl.BlockSpec(memory_space=pltpu.HBM)
    bf16, f32 = jnp.bfloat16, jnp.float32
    held = pl.pallas_call(
        functools.partial(kernel, unit, bounds, later),
        in_specs=[hbm] * 11,
        out_specs=[vmem] * 6,
        out_shape=[
            pltpu.VMEM((points, rows, nodes), f32),
            pltpu.VMEM((blocks + directions * slots + 1, height, LANES), bf16),
            pltpu.VMEM((shares - 1, blocks, height, LANES), bf16),
            pltpu.VMEM((length, 2 * length), bf16),
            pltpu.VMEM((rows, 2 * length), bf16),
            pltpu.VMEM((4, blocks, LANES), f32),
        ],
        scratch_shapes=[
            pltpu.SMEM((directions, slots, halo_list.shape[0]), jnp.int32),
            pltpu.SMEM((count, blocks), jnp.int32),
            pltpu.VMEM((points, rows, nodes), f32),
            pltpu.VMEM((blocks, count, LANES, LANES), bf16),
            pltpu.VMEM((directions, slots, height, LANES), bf16),
            pltpu.VMEM((directions, slots, height, LANES), bf16),
            pltpu.SemaphoreType.DMA((3,)),
            pltpu.SemaphoreType.DMA((7,)),
            pltpu.SemaphoreType.DMA((shares - 1,)),
            pltpu.SemaphoreType.DMA((shares - 1, len(bounds) + len(later) - 4)),
            pltpu.SemaphoreType.DMA((directions,)),
            pltpu.SemaphoreType.DMA((directions,)),
        ]
        + [pltpu.SemaphoreType.REGULAR] * 4,
        compiler_params=pltpu.CompilerParams(
            collective_id=0, has_side_effects=True, vmem_limit_bytes=VMEM_BYTES
        ),
        cost_estimate=pl.CostEstimate(
            flops=2 * height * nodes * (count * LANES + 3 * length),
            bytes_accessed=coupling.size * 2 + 3 * x.size * 4,
            transcendentals=0,
        ),
        name="residual",
    )(
        *[
            pltpu.with_memory_space_constraint(value, pltpu.HBM)
            for value in (
                jnp.transpose(halo_list, (1, 2, 0)),
                neighbour_slot.T,
                x,
                injected,
                coupling,
                synthesis,
                analysis,
                *scales,
            )
        ]
    )
    total, pool, arrived, *tables = (
        pltpu.with_memory_space_constraint(value, pltpu.VMEM) for value in held
    )
    early, token = pl.pallas_call(
        functools.partial(early_kernel, written * LANES),
        in_specs=[vmem],
        out_specs=[hbm, vmem],
        out_shape=[pltpu.HBM((points, rows, nodes), f32), pltpu.VMEM((8, LANES), f32)],
        scratch_shapes=[pltpu.SemaphoreType.DMA((1,))],
        compiler_params=pltpu.CompilerParams(vmem_limit_bytes=1 << 20),
        cost_estimate=pl.CostEstimate(
            flops=0, bytes_accessed=height * written * LANES * 4, transcendentals=0
        ),
        name="early",
    )(total)
    width = nodes - written * LANES
    rest, tail = pl.pallas_call(
        functools.partial(later_kernel, unit, written, later),
        in_specs=[vmem] * 7,
        out_specs=[vmem] * 2,
        out_shape=[
            pltpu.VMEM((points, rows, width), f32),
            pltpu.VMEM((shares, last, height, LANES), bf16),
        ],
        scratch_shapes=[
            pltpu.VMEM((shares - 1, blocks - later[0], height, LANES), bf16),
            pltpu.SemaphoreType.DMA((shares - 1,)),
            pltpu.SemaphoreType.DMA((shares - 1, len(later) - 1)),
        ],
        compiler_params=pltpu.CompilerParams(
            collective_id=1, has_side_effects=True, vmem_limit_bytes=12 << 20
        ),
        cost_estimate=pl.CostEstimate(
            flops=6 * height * width * length, bytes_accessed=0, transcendentals=0
        ),
        name="later",
    )(pltpu.with_memory_space_constraint(token, pltpu.VMEM), total, pool, arrived, *tables)
    total = pl.pallas_call(
        finish_kernel,
        in_specs=[hbm] + [vmem] * 5,
        out_specs=hbm,
        out_shape=pltpu.HBM((points, rows, nodes), f32),
        scratch_shapes=[
            pltpu.VMEM((points, rows, last * LANES), f32),
            pltpu.SemaphoreType.DMA((2,)),
        ],
        input_output_aliases={0: 0},
        compiler_params=pltpu.CompilerParams(vmem_limit_bytes=8 << 20),
        cost_estimate=pl.CostEstimate(
            flops=6 * height * last * LANES * length,
            bytes_accessed=height * width * 4,
            transcendentals=0,
        ),
        name="finish",
    )(
        early,
        *[pltpu.with_memory_space_constraint(value, pltpu.VMEM) for value in (rest, tail)],
        *tables,
    )
    return jnp.transpose(total, (1, 0, 2))


def solution(mesh):
    in_specs = (
        P("harm", None, "node"),
        P("harm", None, "node"),
        P("node", None, None, None),
        P("node"),
        P("node"),
        P("node"),
        P("node"),
        P(),
        P("node", None),
    )
    return jax.shard_map(
        local_part, mesh=mesh, in_specs=in_specs, out_specs=P("harm", None, "node"), check_vma=False
    )
```

```python
import functools

import jax
import jax.numpy as jnp
import numpy as np
from jax import lax
from jax.experimental import pallas as pl
from jax.experimental.pallas import tpu as pltpu
from jax.sharding import PartitionSpec as P

LOG_TWO = 0.6931471805599453
OFFSETS = (-2, -1, 1, 2)
CUTS = (0, 2, 4, 14, 30, 34)
LATER = (34, 40, 44, 46, 48)
TOTAL = 48
LANES = 128
VMEM_BYTES = 36 << 20
MESH = pl.DeviceIdType.MESH


def fourier_tables(length, shares):
    rows = length // shares
    sample = np.arange(length)[:, None]
    column = np.arange(length)[None, :]
    angle = 2.0 * np.pi / length * (column // 2 * sample % length)
    table = np.where(column % 2 == 1, np.sin(angle), np.cos(angle))
    table = np.where(column == 1, np.where(sample % 2 == 0, 1.0, -1.0), table)
    weights = np.where(np.arange(length) < 2, 1.0, 2.0) / length
    analysis = table.T * weights[:, None]
    pulsation = np.arange(length // 2)[:, None, None] / (length // 2)
    pairs = analysis.reshape(length // 2, 2, length)
    slope = np.concatenate([pulsation * pairs[:, 1:], -pulsation * pairs[:, :1]], axis=1)
    both = np.concatenate([analysis, slope.reshape(length, length)], axis=1)
    table = table.astype(np.float32)
    high = table.astype(jnp.bfloat16)
    low = (table - high.astype(np.float32)).astype(jnp.bfloat16)
    order = [
        np.concatenate([np.arange(rows) + (me - by) % shares * rows for by in range(shares)])
        for me in range(shares)
    ]
    synthesis = np.stack([np.concatenate([high[:, o], low[:, o]], axis=1) for o in order])
    return synthesis, both.astype(jnp.bfloat16).reshape(shares, rows, 2 * length)


def evaluate(spectra, synthesis, analysis, saturation, steepness, junction):
    stacked = jnp.concatenate(spectra + spectra, axis=0)
    voltage = jnp.dot(synthesis, stacked, preferred_element_type=jnp.float32)
    drive = steepness * voltage
    softplus = jnp.maximum(drive, 0.0) + jnp.log(1.0 + jnp.exp(-jnp.abs(drive)))
    current = (saturation * (softplus - LOG_TWO)).astype(jnp.bfloat16)
    charge = (junction * voltage * lax.rsqrt(1.0 + voltage * voltage)).astype(jnp.bfloat16)
    samples = jnp.concatenate([current, charge], axis=0)
    return jnp.dot(analysis, samples, preferred_element_type=jnp.float32)


def widen(scale_ref, index, blocks):
    parts = [scale_ref[index, pl.ds(block, 1), :] for block in blocks]
    return jnp.concatenate(parts, axis=1)


def early_kernel(width, total_ref, out_hbm, token_ref, sem):
    copy = pltpu.make_async_copy(
        total_ref.at[:, :, :width], out_hbm.at[:, :, :width], sem.at[0]
    )
    copy.start()
    token_ref[...] = jnp.zeros_like(token_ref)
    copy.wait()


def finish_kernel(
    _, rest_ref, tail_ref, synthesis_ref, analysis_ref, scale_ref, out_hbm, last_ref, sem
):
    points, rows, width = rest_ref.shape
    shares, unit = tail_ref.shape[:2]
    nodes = out_hbm.shape[2]
    blocks = nodes // LANES
    done, before = width - unit * LANES, nodes - width
    bulk = pltpu.make_async_copy(
        rest_ref.at[:, :, :done], out_hbm.at[:, :, before : before + done], sem.at[0]
    )
    bulk.start()
    ids = range(blocks - unit, blocks)
    scales = [widen(scale_ref, index, ids) for index in (1, 2, 3)]
    for point in range(points):
        held = slice(point * rows, (point + 1) * rows)
        spectra = [
            jnp.concatenate([tail_ref[share, inner, held, :] for inner in range(unit)], axis=1)
            for share in range(shares)
        ]
        last_ref[point] = rest_ref[point, :, done:] + evaluate(
            spectra, synthesis_ref[...], analysis_ref[...], *scales
        )
    copy = pltpu.make_async_copy(last_ref, out_hbm.at[:, :, before + done :], sem.at[1])
    copy.start()
    bulk.wait()
    copy.wait()


def later_kernel(
    unit,
    written,
    bounds,
    _,
    total_ref,
    pool_ref,
    before_ref,
    synthesis_ref,
    analysis_ref,
    scale_ref,
    rest_ref,
    tail_ref,
    arrived_ref,
    send_sem,
    recv_sem,
):
    points, rows, nodes = total_ref.shape
    blocks = nodes // LANES
    shares = lax.axis_size("harm")
    me = lax.axis_index("harm")
    base = bounds[0]
    late = lax.rem(lax.axis_index("node"), 2) == 1
    final = bounds[-2]

    def exchange(low, high, by, recv):
        return pltpu.make_async_remote_copy(
            src_ref=pool_ref.at[low:high],
            dst_ref=arrived_ref.at[by - 1, low - base : high - base],
            send_sem=send_sem.at[by - 1],
            recv_sem=recv_sem.at[by - 1, recv],
            device_id={"harm": lax.rem(me + by, shares)},
            device_id_type=MESH,
        )

    pieces = list(zip(bounds[:-1], bounds[1:]))

    def nonlinear(source_ref, shift, group, carry):
        ids = [group * unit + inner for inner in range(unit)]
        factors = [widen(scale_ref, index, ids) for index in (1, 2, 3)]
        width = unit * LANES
        span = pl.ds(pl.multiple_of(group * width, width), width)
        target = pl.ds(pl.multiple_of(group * width - written * LANES, width), width)
        for point in range(points):
            held = slice(point * rows, (point + 1) * rows)
            spectra = [jnp.concatenate([pool_ref[block, held, :] for block in ids], axis=1)]
            for by in range(1, shares):
                spectra.append(
                    jnp.concatenate(
                        [source_ref[by - 1, block - shift, held, :] for block in ids], axis=1
                    )
                )
            rest_ref[point, :, target] = total_ref[point, :, span] + evaluate(
                spectra, synthesis_ref[...], analysis_ref[...], *factors
            )
        return carry

    @pl.when(late)
    def _():
        barrier = pltpu.get_barrier_semaphore()
        for by in range(1, shares):
            pl.semaphore_signal(
                barrier, inc=1, device_id={"harm": lax.rem(me + by, shares)}, device_id_type=MESH
            )
        pl.semaphore_wait(barrier, shares - 1)
        for index, (low, high) in enumerate(pieces):
            for by in range(1, shares):
                exchange(low, high, by, index).start()
        lax.fori_loop(
            written // unit, base // unit, functools.partial(nonlinear, before_ref, 0), 0
        )
        rest_ref[:, :, (final - written) * LANES :] = total_ref[:, :, final * LANES :]
        tail_ref[0] = pool_ref[final:blocks]
        for index, (low, high) in enumerate(pieces):
            for by in range(1, shares):
                exchange(low, high, by, index).wait_recv()
            if high < blocks:
                lax.fori_loop(
                    low // unit, high // unit, functools.partial(nonlinear, arrived_ref, base), 0
                )
        for by in range(1, shares):
            tail_ref[by] = arrived_ref[by - 1, final - base :]
        for by in range(1, shares):
            exchange(base, blocks, by, 0).wait_send()

    @pl.when(jnp.logical_not(late))
    def _():
        rest_ref[...] = total_ref[:, :, written * LANES :]
        tail_ref[0] = pool_ref[final:blocks]
        for by in range(1, shares):
            tail_ref[by] = before_ref[by - 1, final:blocks]


def kernel(
    unit,
    bounds,
    later,
    list_hbm,
    slot_hbm,
    x_hbm,
    source_hbm,
    coupling_hbm,
    synthesis_hbm,
    analysis_hbm,
    capacitance_hbm,
    saturation_hbm,
    steepness_hbm,
    junction_hbm,
    out_ref,
    pool_ref,
    arrived_ref,
    synthesis_ref,
    analysis_ref,
    scale_ref,
    list_ref,
    slot_ref,
    x_ref,
    coupling_ref,
    packed_ref,
    halo_ref,
    x_sem,
    local_sem,
    send_sem,
    recv_sem,
    halo_send_sem,
    halo_recv_sem,
    ready_sem,
    start_sem,
    group_sem,
    halo_sem,
):
    points, rows, nodes = x_ref.shape
    blocks = nodes // LANES
    chunks = len(bounds) - 1
    loads = bounds[:3] + [blocks]
    groups = bounds[:1] + bounds[3:] + later[1:]
    count, slots = coupling_ref.shape[1], list_ref.shape[1]
    shares, devices = lax.axis_size("harm"), lax.axis_size("node")
    me, place = lax.axis_index("harm"), lax.axis_index("node")
    length = rows * shares

    def on_mesh(device):
        return jnp.logical_and(device >= 0, device < devices)

    def load(step):
        span = slice(loads[step] * LANES, loads[step + 1] * LANES)
        return pltpu.make_async_copy(
            x_hbm.at[:, :, span], x_ref.at[:, :, span], x_sem.at[step]
        )

    def exchange(low, high, by, recv):
        return pltpu.make_async_remote_copy(
            src_ref=pool_ref.at[low:high],
            dst_ref=arrived_ref.at[by - 1, low:high],
            send_sem=send_sem.at[by - 1],
            recv_sem=recv_sem.at[by - 1, recv],
            device_id={"harm": lax.rem(me + by, shares)},
            device_id_type=MESH,
        )

    def group_of(block):
        return sum(block >= end for end in groups[1:])

    def arrival(group, by):
        return exchange(groups[group], groups[group + 1], by, group)

    def halo(direction, device):
        return pltpu.make_async_remote_copy(
            src_ref=packed_ref.at[direction],
            dst_ref=halo_ref.at[direction],
            send_sem=halo_send_sem.at[direction],
            recv_sem=halo_recv_sem.at[direction],
            device_id={"node": device},
            device_id_type=MESH,
        )

    root = me == 0
    member = jnp.logical_not(root)
    members = [{"harm": other} for other in range(1, shares)]
    barrier = pltpu.get_barrier_semaphore()
    load(0).start()

    def signal(semaphore, device):
        pl.semaphore_signal(semaphore, inc=1, device_id=device, device_id_type=MESH)

    @pl.when(root)
    def _():
        for other in members:
            signal(barrier, other)

    def greet(semaphore):
        for offset in OFFSETS:

            @pl.when(jnp.logical_and(root, on_mesh(place + offset)))
            def _():
                signal(semaphore, {"node": place + offset})

    greet(barrier)
    greeted = sum(on_mesh(place + offset).astype(jnp.int32) for offset in OFFSETS)
    for step in range(1, len(loads) - 1):
        load(step).start()
    tables = [
        pltpu.make_async_copy(source, target, local_sem.at[i])
        for i, (source, target) in enumerate([(list_hbm, list_ref), (slot_hbm, slot_ref)])
    ]
    large = [
        pltpu.make_async_copy(source, target, local_sem.at[i + 2])
        for i, (source, target) in enumerate(
            [
                (source_hbm, out_ref),
                (coupling_hbm, coupling_ref),
                (synthesis_hbm.at[me], synthesis_ref),
                (analysis_hbm.at[me], analysis_ref),
            ]
        )
    ]
    scales = [
        pltpu.make_async_copy(source, scale_ref.at[i], local_sem.at[6])
        for i, source in enumerate([capacitance_hbm, saturation_hbm, steepness_hbm, junction_hbm])
    ]
    for copy in tables:
        copy.start()

    def round_block(block, carry):
        span = pl.ds(pl.multiple_of(block * LANES, LANES), LANES)
        for point in range(points):
            pool_ref[block, point * rows : (point + 1) * rows, :] = x_ref[point, :, span].astype(
                jnp.bfloat16
            )
        return carry

    def round_chunk(chunk):
        if chunk < len(loads) - 1:
            load(chunk).wait()
        lax.fori_loop(bounds[chunk], bounds[chunk + 1], round_block, 0, unroll=unit)

    def send(low, high):
        for by in range(1, shares):
            exchange(low, high, by, group_of(low)).start()

    @pl.when(member)
    def _():
        pl.semaphore_wait(barrier, 1)
        signal(ready_sem, {"harm": 0})

    def start_large():
        for copy in large + scales:
            copy.start()

    round_chunk(0)
    round_chunk(1)

    @pl.when(root)
    def _():
        start_large()
        pl.semaphore_wait(barrier, greeted)
        pl.semaphore_wait(ready_sem, shares - 1)
        if shares > 2:
            for other in members:
                signal(start_sem, other)

    if shares > 2:

        @pl.when(member)
        def _():
            pl.semaphore_wait(start_sem, 1)

    send(bounds[0], bounds[1])
    pl.when(member)(start_large)
    send(bounds[1], bounds[2])
    for chunk in range(2, chunks):
        round_chunk(chunk)
        if chunk > 2:
            send(bounds[chunk - 1], bounds[chunk])
    lax.fori_loop(bounds[-1], blocks, round_block, 0, unroll=unit)
    for copy in tables:
        copy.wait()
    for direction in range(len(OFFSETS)):
        for slot in range(slots):
            packed_ref[direction, slot] = pool_ref[list_ref[direction, slot, place]]
    late = lax.rem(place, 2) == 1
    soon = jnp.logical_not(late)
    send(bounds[-2], bounds[-1])

    @pl.when(soon)
    def _():
        for low, high in zip(later[:-1], later[1:]):
            send(low, high)

    greet(group_sem)

    @pl.when(root)
    def _():
        pl.semaphore_wait(group_sem, greeted)
        for other in members:
            signal(halo_sem, other)

    @pl.when(member)
    def _():
        pl.semaphore_wait(halo_sem, 1)

    for direction, offset in enumerate(OFFSETS):

        @pl.when(on_mesh(place + offset))
        def _():
            halo(direction, place + offset).start()

    pool_ref[blocks + len(OFFSETS) * slots] = jnp.zeros(pool_ref.shape[1:], pool_ref.dtype)
    for copy in large:
        copy.wait()
    pltpu.make_async_copy(scale_ref, scale_ref, local_sem.at[6]).wait()
    for direction, offset in enumerate(OFFSETS):
        first = blocks + direction * slots
        there = on_mesh(place - offset)

        @pl.when(there)
        def _():
            halo(direction, place - offset).wait_recv()
            for slot in range(slots):
                pool_ref[first + slot] = halo_ref[direction, slot]

        @pl.when(jnp.logical_not(there))
        def _():
            for slot in range(slots):
                pool_ref[first + slot] = jnp.zeros(pool_ref.shape[1:], pool_ref.dtype)

    row = me * rows + lax.broadcasted_iota(jnp.int32, (rows, LANES), 0)
    even = row % 2 == 0
    rate = (row // 2).astype(jnp.float32) * (2.0 / length)
    rate = jnp.where(even, rate, -rate)

    def couple(block, carry):
        gathered = jnp.concatenate([pool_ref[slot_ref[k, block]] for k in range(count)], axis=1)
        matrix = jnp.concatenate([coupling_ref[block, k] for k in range(count)], axis=1)
        coupled = lax.dot_general(
            gathered, matrix, (((1,), (1,)), ((), ())), preferred_element_type=jnp.float32
        )
        scaled = rate * scale_ref[0, pl.ds(block, 1), :]
        span = pl.ds(pl.multiple_of(block * LANES, LANES), LANES)
        for point in range(points):
            values = x_ref[point, :, span]
            other = jnp.where(even, pltpu.roll(values, rows - 1, 0), pltpu.roll(values, 1, 0))
            out_ref[point, :, span] = (
                coupled[point * rows : (point + 1) * rows]
                + scaled * other
                - out_ref[point, :, span]
            )
        return carry

    lax.fori_loop(0, blocks, couple, 0, unroll=unit)

    def nonlinear(group, carry):
        ids = [group * unit + inner for inner in range(unit)]
        factors = [widen(scale_ref, index, ids) for index in (1, 2, 3)]
        span = pl.ds(pl.multiple_of(group * unit * LANES, unit * LANES), unit * LANES)
        for point in range(points):
            held = slice(point * rows, (point + 1) * rows)
            spectra = [jnp.concatenate([pool_ref[block, held, :] for block in ids], axis=1)]
            for by in range(1, shares):
                spectra.append(
                    jnp.concatenate([arrived_ref[by - 1, block, held, :] for block in ids], axis=1)
                )
            out_ref[point, :, span] += evaluate(
                spectra, synthesis_ref[...], analysis_ref[...], *factors
            )
        return carry

    def receive(group):
        for by in range(1, shares):
            arrival(group, by).wait_recv()

    def process(group):
        lax.fori_loop(groups[group] // unit, groups[group + 1] // unit, nonlinear, 0)

    shared = groups.index(bounds[-1]) - 1
    for group in range(shared):
        receive(group)
        process(group)
    receive(shared)

    @pl.when(soon)
    def _():
        process(shared)
        for group in range(shared + 1, len(groups) - 1):
            receive(group)
            if group < len(groups) - 2:
                process(group)
        for by in range(1, shares):
            exchange(0, blocks, by, 0).wait_send()

    @pl.when(late)
    def _():
        for by in range(1, shares):
            exchange(0, bounds[-1], by, 0).wait_send()

    for direction, offset in enumerate(OFFSETS):

        @pl.when(on_mesh(place + offset))
        def _():
            halo(direction, place + offset).wait_send()


def local_part(
    spectrum,
    source,
    coupling,
    capacitance,
    saturation,
    steepness,
    junction,
    halo_list,
    neighbour_slot,
):
    rows, points, nodes = spectrum.shape
    shares = lax.axis_size("harm")
    length = rows * shares
    blocks = nodes // LANES
    unit = 2 if blocks % 2 == 0 else 1
    bounds, later = (
        sorted({cut * blocks // TOTAL // unit * unit for cut in cuts}) for cuts in (CUTS, LATER)
    )
    later[-1] = blocks
    last, written = blocks - later[-2], bounds[-2]
    slots, count = halo_list.shape[2], neighbour_slot.shape[1]
    directions = len(OFFSETS)
    height = points * rows
    x = jnp.transpose(spectrum, (1, 0, 2))
    injected = jnp.transpose(source, (1, 0, 2))
    synthesis, analysis = (jnp.asarray(t) for t in fourier_tables(length, shares))
    scales = [v.reshape(blocks, LANES) for v in (capacitance, saturation, steepness, junction)]
    vmem = pl.BlockSpec(memory_space=pltpu.VMEM)
    hbm = pl.BlockSpec(memory_space=pltpu.HBM)
    bf16, f32 = jnp.bfloat16, jnp.float32
    held = pl.pallas_call(
        functools.partial(kernel, unit, bounds, later),
        in_specs=[hbm] * 11,
        out_specs=[vmem] * 6,
        out_shape=[
            pltpu.VMEM((points, rows, nodes), f32),
            pltpu.VMEM((blocks + directions * slots + 1, height, LANES), bf16),
            pltpu.VMEM((shares - 1, blocks, height, LANES), bf16),
            pltpu.VMEM((length, 2 * length), bf16),
            pltpu.VMEM((rows, 2 * length), bf16),
            pltpu.VMEM((4, blocks, LANES), f32),
        ],
        scratch_shapes=[
            pltpu.SMEM((directions, slots, halo_list.shape[0]), jnp.int32),
            pltpu.SMEM((count, blocks), jnp.int32),
            pltpu.VMEM((points, rows, nodes), f32),
            pltpu.VMEM((blocks, count, LANES, LANES), bf16),
            pltpu.VMEM((directions, slots, height, LANES), bf16),
            pltpu.VMEM((directions, slots, height, LANES), bf16),
            pltpu.SemaphoreType.DMA((3,)),
            pltpu.SemaphoreType.DMA((7,)),
            pltpu.SemaphoreType.DMA((shares - 1,)),
            pltpu.SemaphoreType.DMA((shares - 1, len(bounds) + len(later) - 4)),
            pltpu.SemaphoreType.DMA((directions,)),
            pltpu.SemaphoreType.DMA((directions,)),
        ]
        + [pltpu.SemaphoreType.REGULAR] * 4,
        compiler_params=pltpu.CompilerParams(
            collective_id=0, has_side_effects=True, vmem_limit_bytes=VMEM_BYTES
        ),
        cost_estimate=pl.CostEstimate(
            flops=2 * height * nodes * (count * LANES + 3 * length),
            bytes_accessed=coupling.size * 2 + 3 * x.size * 4,
            transcendentals=0,
        ),
        name="residual",
    )(
        *[
            pltpu.with_memory_space_constraint(value, pltpu.HBM)
            for value in (
                jnp.transpose(halo_list, (1, 2, 0)),
                neighbour_slot.T,
                x,
                injected,
                coupling,
                synthesis,
                analysis,
                *scales,
            )
        ]
    )
    total, pool, arrived, *tables = (
        pltpu.with_memory_space_constraint(value, pltpu.VMEM) for value in held
    )
    early, token = pl.pallas_call(
        functools.partial(early_kernel, written * LANES),
        in_specs=[vmem],
        out_specs=[hbm, vmem],
        out_shape=[pltpu.HBM((points, rows, nodes), f32), pltpu.VMEM((8, LANES), f32)],
        scratch_shapes=[pltpu.SemaphoreType.DMA((1,))],
        compiler_params=pltpu.CompilerParams(vmem_limit_bytes=1 << 20),
        cost_estimate=pl.CostEstimate(
            flops=0, bytes_accessed=height * written * LANES * 4, transcendentals=0
        ),
        name="early",
    )(total)
    width = nodes - written * LANES
    rest, tail = pl.pallas_call(
        functools.partial(later_kernel, unit, written, later),
        in_specs=[vmem] * 7,
        out_specs=[vmem] * 2,
        out_shape=[
            pltpu.VMEM((points, rows, width), f32),
            pltpu.VMEM((shares, last, height, LANES), bf16),
        ],
        scratch_shapes=[
            pltpu.VMEM((shares - 1, blocks - later[0], height, LANES), bf16),
            pltpu.SemaphoreType.DMA((shares - 1,)),
            pltpu.SemaphoreType.DMA((shares - 1, len(later) - 1)),
        ],
        compiler_params=pltpu.CompilerParams(
            collective_id=1, has_side_effects=True, vmem_limit_bytes=12 << 20
        ),
        cost_estimate=pl.CostEstimate(
            flops=6 * height * width * length, bytes_accessed=0, transcendentals=0
        ),
        name="later",
    )(pltpu.with_memory_space_constraint(token, pltpu.VMEM), total, pool, arrived, *tables)
    total = pl.pallas_call(
        finish_kernel,
        in_specs=[hbm] + [vmem] * 5,
        out_specs=hbm,
        out_shape=pltpu.HBM((points, rows, nodes), f32),
        scratch_shapes=[
            pltpu.VMEM((points, rows, last * LANES), f32),
            pltpu.SemaphoreType.DMA((2,)),
        ],
        input_output_aliases={0: 0},
        compiler_params=pltpu.CompilerParams(vmem_limit_bytes=8 << 20),
        cost_estimate=pl.CostEstimate(
            flops=6 * height * last * LANES * length,
            bytes_accessed=height * width * 4,
            transcendentals=0,
        ),
        name="finish",
    )(
        early,
        *[pltpu.with_memory_space_constraint(value, pltpu.VMEM) for value in (rest, tail)],
        *tables,
    )
    return jnp.transpose(total, (1, 0, 2))


def solution(mesh):
    in_specs = (
        P("harm", None, "node"),
        P("harm", None, "node"),
        P("node", None, None, None),
        P("node"),
        P("node"),
        P("node"),
        P("node"),
        P(),
        P("node", None),
    )
    return jax.shard_map(
        local_part, mesh=mesh, in_specs=in_specs, out_specs=P("harm", None, "node"), check_vma=False
    )
```
